32 devices in a mesh: dp: 2 (over x), tp: 4 (over z), sp: 4 (over y, core).
Axes of the slice: x: 2, y: 2, z: 4, core: 2. Of those that a mesh axis runs over, the one named last changes fastest.
Arguments:
- x_seq: bfloat16 [16384, 2304], P(('dp', 'sp', 'tp')), parts along dimension 0
- w_query: bfloat16 [2304, 8, 256], P(None, 'tp')
- w_key: bfloat16 [2304, 4, 256], P(None, 'tp')
- w_value: bfloat16 [2304, 4, 256], P(None, 'tp')
- w_out: bfloat16 [8, 256, 2304], P('tp')
Outputs:
- output: bfloat16 [16384, 2304], P(('dp', 'sp', 'tp')), parts along dimension 0
There are 2 independent parts. The reference program is written for one: setup_inputs(seed, part) draws one part's arguments, and reference() takes and returns one part's arrays. A program takes and returns all parts, laid end to end along the dimension named above; an argument that names none is the same for every part.
All inputs are finite; a program needn't handle non-finite values.
Results may differ from the reference program's by a relative error of at most 0.00549951.
Values are sent between devices in bfloat16 or wider.
A program may use at most 1 GiB of HBM per device.

```python
import jax
import jax.numpy as jnp
from jax import lax

D = 2304
HEADS = 8
KV_HEADS = 4
HEAD = 256
WINDOW = 4096
CHUNK = 1024
SP = 4
QBLOCK = 128

SEQ = 2 * SP * CHUNK
GROUP = HEADS // KV_HEADS
SPAN = WINDOW + QBLOCK
NEG_BIG = -1e30


def setup_inputs(seed: int = 0, part: int = 0) -> dict:
    base_key = jax.random.key(seed)
    part_key = jax.random.fold_in(base_key, part)
    weight_keys = jax.random.split(base_key, 4)
    x_rows = jax.random.normal(part_key, (SEQ, D), jnp.float32)
    w_query = jax.random.normal(weight_keys[0], (D, HEADS, HEAD), jnp.float32) * (1.5 * D ** -0.5)
    w_key = jax.random.normal(weight_keys[1], (D, KV_HEADS, HEAD), jnp.float32) * D ** -0.5
    w_value = jax.random.normal(weight_keys[2], (D, KV_HEADS, HEAD), jnp.float32) * D ** -0.5
    w_out = jax.random.normal(weight_keys[3], (HEADS, HEAD, D), jnp.float32) * (HEADS * HEAD) ** -0.5
    return {"x_seq": x_rows.astype(jnp.bfloat16), "w_query": w_query.astype(jnp.bfloat16), "w_key": w_key.astype(jnp.bfloat16), "w_value": w_value.astype(jnp.bfloat16), "w_out": w_out.astype(jnp.bfloat16)}


def to_natural(rows_in):
    blocks = rows_in.reshape((SP, 2, CHUNK) + rows_in.shape[1:])
    return jnp.concatenate([blocks[:, 0], blocks[::-1, 1]], axis=0).reshape(rows_in.shape)


def to_stored(rows_in):
    blocks = rows_in.reshape((2 * SP, CHUNK) + rows_in.shape[1:])
    return jnp.stack([blocks[:SP], blocks[SP:][::-1]], axis=1).reshape(rows_in.shape)


def reference(x_seq, w_query, w_key, w_value, w_out):
    x_nat = to_natural(x_seq)
    q_all = jnp.dot(x_nat, w_query.reshape(D, HEADS * HEAD), preferred_element_type=jnp.float32).astype(jnp.bfloat16).reshape(SEQ, KV_HEADS, GROUP, HEAD)
    k_all = jnp.dot(x_nat, w_key.reshape(D, KV_HEADS * HEAD), preferred_element_type=jnp.float32).astype(jnp.bfloat16).reshape(SEQ, KV_HEADS, HEAD)
    v_all = jnp.dot(x_nat, w_value.reshape(D, KV_HEADS * HEAD), preferred_element_type=jnp.float32).astype(jnp.bfloat16).reshape(SEQ, KV_HEADS, HEAD)
    zero_front = jnp.zeros((WINDOW, KV_HEADS, HEAD), jnp.bfloat16)
    k_pad = jnp.concatenate([zero_front, k_all], axis=0)
    v_pad = jnp.concatenate([zero_front, v_all], axis=0)
    score_scale = HEAD ** -0.5
    row_ids = jnp.arange(QBLOCK)[:, None]
    col_ids = jnp.arange(SPAN)[None, :]

    def one_block(start):
        q_blk = lax.dynamic_slice_in_dim(q_all, start, QBLOCK, 0).astype(jnp.float32)
        k_blk = lax.dynamic_slice_in_dim(k_pad, start, SPAN, 0).astype(jnp.float32)
        v_blk = lax.dynamic_slice_in_dim(v_pad, start, SPAN, 0).astype(jnp.float32)
        scores = jnp.einsum("qhgd,khd->hgqk", q_blk, k_blk) * score_scale
        pos_gap = WINDOW + row_ids - col_ids
        visible = (pos_gap >= 0) & (pos_gap < WINDOW) & (start - WINDOW + col_ids >= 0)
        scores = jnp.where(visible, scores, NEG_BIG)
        row_max = jnp.max(scores, axis=-1, keepdims=True)
        prob_blk = jnp.where(visible, jnp.exp(scores - row_max), 0.0)
        row_denom = jnp.sum(prob_blk, axis=-1)
        weighted = jnp.einsum("hgqk,khd->hgqd", prob_blk.astype(jnp.bfloat16).astype(jnp.float32), v_blk)
        normed = (weighted / row_denom[..., None]).astype(jnp.bfloat16)
        return jnp.transpose(normed, (2, 0, 1, 3)).reshape(QBLOCK, HEADS * HEAD)

    starts = jnp.arange(SEQ // QBLOCK) * QBLOCK
    o_nat = lax.map(one_block, starts).reshape(SEQ, HEADS * HEAD)
    y_nat = jnp.dot(o_nat, w_out.reshape(HEADS * HEAD, D), preferred_element_type=jnp.float32).astype(jnp.bfloat16)
    return to_stored(y_nat)
```

```python
import jax
import jax.numpy as jnp
from jax import lax
from jax.experimental import pallas as pl
from jax.experimental.pallas import tpu as pltpu
from jax.sharding import PartitionSpec as P


LOG2E = 1.4426950408889634


HB = 512
HD = 256
NSUB = 4


def attn_kernel(info_ref, *refs):
    q_in, q_shipped, kv_in = refs[:4], refs[4:7], refs[7:23]
    o_ref = refs[23]
    q_all, kv_all, m_ref, l_ref, acc_ref, qsem, ksem = refs[24:]
    z, r = info_ref[0], info_ref[1]
    low = (z < 2).astype(jnp.int32)
    zx = jnp.where(z % 2 == 0, z + 1, z - 1)
    t_ids = (z, zx, jnp.where(low == 1, 2, 1), jnp.where(low == 1, 3, 0))

    def half_id(t, rr):
        return jnp.where(t < 2, 2 * rr + t, 2 * (7 - rr) + t - 2)

    r1 = jnp.where(r % 2 == 0, r + 1, r - 1)
    r2 = jnp.where(r < 2, r + 2, r - 2)
    r3 = 3 - r
    copies = [pltpu.make_async_copy(q_in[0].at[:, 2 * HD:], q_all.at[t_ids[0]], qsem.at[0])]
    inner = (z == 1) | (z == 2)
    for j in range(1, 4):

        @pl.when(inner)
        def _():
            pltpu.make_async_copy(q_in[j].at[:, 2 * HD:], q_all.at[t_ids[j]], qsem.at[j]).start()

        @pl.when(jnp.logical_not(inner))
        def _():
            pltpu.make_async_copy(q_shipped[j - 1], q_all.at[t_ids[j]], qsem.at[j]).start()

    for j in range(4):
        for k, rr in enumerate((r, r1, r2, r3)):
            copies.append(pltpu.make_async_copy(kv_in[4 * j + k], kv_all.at[half_id(t_ids[j], rr)], ksem.at[4 * j + k]))
    for c in copies:
        c.start()
    for c in copies:
        c.wait()
    for j in range(1, 4):
        pltpu.make_async_copy(q_shipped[j - 1], q_all.at[t_ids[j]], qsem.at[j]).wait()

    scale = LOG2E * HD ** -0.5
    rows = 2 * HB // NSUB

    def block(t, g, mode):
        k_blk = kv_all[g, :, 0:HD]
        v_blk = kv_all[g, :, HD:2 * HD]
        for sub in range(NSUB):
            head, off = divmod(sub * rows, HB)
            rs = pl.ds(sub * rows, rows)
            q_sub = q_all[t, pl.ds(off, rows), head * HD:(head + 1) * HD]
            s = lax.dot_general(q_sub, k_blk, (((1,), (1,)), ((), ())), preferred_element_type=jnp.float32)
            if mode != "full":
                row = lax.broadcasted_iota(jnp.int32, (rows, HB), 0) + off
                col = lax.broadcasted_iota(jnp.int32, (rows, HB), 1)
                keep = (col <= row) if mode == "diag" else (col > row)
                s = jnp.where(keep, s, -jnp.inf)
            m_cur = jnp.max(s, axis=1, keepdims=True)
            if mode == "diag":
                m_new = jnp.broadcast_to(m_cur, (rows, 128))
            else:
                m_old = m_ref[rs, :]
                m_new = jnp.maximum(m_old, m_cur)
                alpha = jnp.exp2((m_old - m_new) * scale)
            p = jnp.exp2((s - m_new[:, 0:1]) * scale)
            l_new = p[:, 0:128] + p[:, 128:256] + p[:, 256:384] + p[:, 384:512]
            pv = jnp.dot(p.astype(jnp.bfloat16), v_blk, preferred_element_type=jnp.float32)
            m_ref[rs, :] = m_new
            if mode == "diag":
                l_ref[rs, :] = l_new
                acc_ref[rs, :] = pv
            else:
                l_ref[rs, :] = l_ref[rs, :] * alpha + l_new
                acc_ref[rs, :] = acc_ref[rs, :] * jnp.concatenate([alpha, alpha], axis=1) + pv

    def one_piece(t, carry):
        g = half_id(t, r)
        block(t, g, "diag")

        def full_step(kb, c):
            block(t, kb, "full")
            return c

        lax.fori_loop(jnp.maximum(g - 7, 0), g, full_step, 0)

        @pl.when(g >= 8)
        def _():
            block(t, g - 8, "edge")

        for sub in range(NSUB):
            head, off = divmod(sub * rows, HB)
            rs = pl.ds(sub * rows, rows)
            total = jnp.sum(l_ref[rs, :], axis=1, keepdims=True)
            o_ref[t, pl.ds(off, rows), head * HD:(head + 1) * HD] = (acc_ref[rs, :] / total).astype(jnp.bfloat16)
        return carry

    lax.fori_loop(0, 4, one_piece, 0)


def attention(info, ps, qs, kvs):
    any_spec = pl.BlockSpec(memory_space=pl.ANY)
    return pl.pallas_call(
        attn_kernel,
        out_shape=jax.ShapeDtypeStruct((4, HB, 2 * HD), jnp.bfloat16),
        in_specs=[pl.BlockSpec(memory_space=pltpu.SMEM)] + [any_spec] * 23,
        out_specs=pl.BlockSpec(memory_space=pltpu.VMEM),
        scratch_shapes=[
            pltpu.VMEM((4, HB, 2 * HD), jnp.bfloat16),
            pltpu.VMEM((16, HB, 2 * HD), jnp.bfloat16),
            pltpu.VMEM((2 * HB, 128), jnp.float32),
            pltpu.VMEM((2 * HB, 128), jnp.float32),
            pltpu.VMEM((2 * HB, HD), jnp.float32),
            pltpu.SemaphoreType.DMA((4,)),
            pltpu.SemaphoreType.DMA((16,)),
        ],
        compiler_params=pltpu.CompilerParams(vmem_limit_bytes=48 * 1024 * 1024),
        cost_estimate=pl.CostEstimate(flops=17_000_000_000, bytes_accessed=12_000_000, transcendentals=16_000_000),
        name="window_attention",
    )(info, *ps, *qs, *kvs)


def out_kernel(info_ref, o0, o1, o2, o3, w0, w1, w2, w3, y_ref):
    total = jnp.dot(o0[...], w0[0], preferred_element_type=jnp.float32)
    for o_ref, w_ref in ((o1, w1), (o2, w2), (o3, w3)):
        total = total + jnp.dot(o_ref[...], w_ref[0], preferred_element_type=jnp.float32)
    y_ref[...] = total.astype(y_ref.dtype)


def out_project(info, pieces, w_full):
    d_model = w_full.shape[2]
    tile = 384
    piece_spec = pl.BlockSpec((HB, 2 * HD), lambda n, info: (0, 0))

    def w_spec(k):
        return pl.BlockSpec((1, 2 * HD, tile), lambda n, info: (info[2 + k], 0, n))

    return pl.pallas_call(
        out_kernel,
        out_shape=jax.ShapeDtypeStruct((HB, d_model), jnp.bfloat16),
        grid_spec=pltpu.PrefetchScalarGridSpec(
            num_scalar_prefetch=1,
            grid=(d_model // tile,),
            in_specs=[piece_spec] * 4 + [w_spec(k) for k in range(4)],
            out_specs=pl.BlockSpec((HB, tile), lambda n, info: (0, n)),
        ),
        compiler_params=pltpu.CompilerParams(vmem_limit_bytes=32 * 1024 * 1024),
        cost_estimate=pl.CostEstimate(flops=4_800_000_000, bytes_accessed=14_000_000, transcendentals=0),
        name="out_project",
    )(info, *pieces, w_full, w_full, w_full, w_full)


def solution(mesh):
    def sublayer(x, w_query, w_key, w_value, w_out):
        d_model = x.shape[1]
        z, r, dp = lax.axis_index("tp"), lax.axis_index("sp"), lax.axis_index("dp")
        inner = (z == 1) | (z == 2)
        n_part = mesh.shape["dp"] * mesh.shape["sp"]
        my_part = dp * mesh.shape["sp"] + r
        info = jnp.stack([z, r, z, z ^ 1, z ^ 2, z ^ 3]).astype(jnp.int32)

        def dot(a, b):
            return jnp.dot(a, b, preferred_element_type=jnp.float32).astype(jnp.bfloat16)

        from_edge = lax.ppermute(x, "tp", [(0, 1), (3, 2)])
        from_inner = lax.ppermute(x, "tp", [(1, 2), (2, 1)])
        from_far = lax.ppermute(from_edge, "tp", [(1, 2), (2, 1)])

        w_own = jnp.concatenate([w_key.reshape(d_model, HD), w_value.reshape(d_model, HD), w_query.reshape(d_model, 2 * HD)], axis=1)
        part = d_model // n_part
        w_part = lax.dynamic_slice_in_dim(w_own, my_part * part, part, 0)
        w_part = lax.ppermute(w_part, "tp", [(0, 1), (3, 2)])
        w_edge = lax.all_gather(w_part, ("dp", "sp"), axis=0, tiled=True)

        p_own = dot(x, w_own)
        p_b_in = dot(from_edge, w_own)
        p_c_in = dot(from_inner, w_own)
        p_d_in = dot(from_far, w_own)
        kv_own = p_own[:, :2 * HD]

        def ship(src, mine):
            made = dot(src, w_edge)
            kv = lax.ppermute(made[:, :2 * HD], "tp", [(1, 0), (2, 3)])
            q = lax.ppermute(made[:, 2 * HD:], "tp", [(1, 0), (2, 3)])
            return jnp.where(inner, mine[:, :2 * HD], kv), q

        kv_b, q_b = ship(x, p_b_in)
        kv_c, q_c = ship(from_inner, p_c_in)
        kv_d, q_d = ship(from_far, p_d_in)

        def spread(kv):
            across = lax.ppermute(kv, "sp", [(0, 2), (1, 3), (2, 0), (3, 1)])
            mate = lax.ppermute(kv, "sp", [(0, 1), (1, 0), (2, 3), (3, 2)])
            mate_across = lax.ppermute(across, "sp", [(0, 1), (1, 0), (2, 3), (3, 2)])
            return kv, mate, across, mate_across

        kvs = spread(kv_own) + spread(kv_b) + spread(kv_c) + spread(kv_d)
        o = attention(info, (p_own, p_b_in, p_c_in, p_d_in), (q_b, q_c, q_d), kvs)

        wo_rows = w_out.reshape(2 * HD, d_model)
        wo_part = lax.dynamic_slice_in_dim(wo_rows, my_part * (2 * HD // n_part), 2 * HD // n_part, 0)
        wo_full = lax.all_gather(wo_part, ("tp", "dp", "sp"), axis=0, tiled=True).reshape(4, 2 * HD, d_model)

        def o_for(k):
            return lax.dynamic_index_in_dim(o, z ^ k, 0, keepdims=False)

        pieces = [o_for(0)]
        for k in range(1, 4):
            pieces.append(lax.ppermute(o_for(k), "tp", [(i, i ^ k) for i in range(4)]))
        return out_project(info, pieces, wo_full)

    return jax.shard_map(sublayer, mesh=mesh, in_specs=(P(("dp", "sp", "tp"), None), P(None, "tp", None), P(None, "tp", None), P(None, "tp", None), P("tp", None, None)), out_specs=P(("dp", "sp", "tp"), None), check_vma=False)
```

```python
import functools

import jax
import jax.numpy as jnp
from jax import lax
from jax.experimental import pallas as pl
from jax.experimental.pallas import tpu as pltpu
from jax.sharding import PartitionSpec as P

LOG2E = 1.4426950408889634
WINDOW = 4096
NEG_BIG = -1e30
MESH = pl.DeviceIdType.MESH

HB = 512
HD = 256
HW = 2 * HD
SUB = 256

E1, C1, C2 = 0, 2, 3
WZ, WY, WX, WXY, WC = 5, 6, 7, 8, 9
SHIP_KV, SHIP_Q = 13, 16
SP_Y, SP_OWN, SP_FAR = 19, 23, 27
OZ, OY, OX, OXY, OC = 30, 34, 35, 36, 37
HOME = 40
N_TX = 44


def sublayer_kernel(x_ref, w_ref, wo_ref, y_ref, xbuf, wbuf, webuf, q_buf, kv_buf, made, m_ref, l_ref, acc_ref, o_buf, o_recv, wo_buf, send_sem, recv_sem, load_sem):
    z, r, dp = lax.axis_index("tp"), lax.axis_index("sp"), lax.axis_index("dp")
    z_by = (z, z + 1 - 2 * (z % 2), z + 2 - 4 * (z // 2), 3 - z)
    r1, r2 = r + 1 - 2 * (r % 2), r + 2 - 4 * (r // 2)
    inner = ((z + 1) // 2) % 2
    is_inner, is_edge = inner == 1, inner == 0
    d_model = xbuf.shape[2]
    w_rows, o_rows = d_model // 8, HW // 8

    t_c = inner * (3 - z) + (1 - inner) * z_by[2]
    t_d = inner * z_by[2] + (1 - inner) * (3 - z)
    t_of = (z, z_by[1], t_c, t_d)

    def half_id(t, rr):
        return t + 2 * rr + (t // 2) * (12 - 4 * rr)

    def to(**axes):
        return axes

    over_z = tuple(to(tp=z_by[k]) for k in range(4))
    over_core, over_y, over_x = to(sp=r1), to(sp=r2), to(dp=1 - dp)

    def tx(idx, src, dst, device):
        return pltpu.make_async_remote_copy(src_ref=src, dst_ref=dst, send_sem=send_sem.at[idx], recv_sem=recv_sem.at[idx], device_id=device, device_id_type=MESH)

    def send(idx, src, dst, device):
        tx(idx, src, dst, device).start()

    def arrived(idx, dst):
        tx(idx, dst, dst, over_core).wait_recv()

    def sent(idx, src):
        tx(idx, src, src, over_core).wait_send()

    def rows(n, size):
        return pl.ds(pl.multiple_of(n * size, size), size)

    x_half = [pl.ds(0, HB // 2), pl.ds(HB // 2, HB // 2)]
    piece = dp * 4 + r
    p_y, p_x, p_xy = dp * 4 + r2, (1 - dp) * 4 + r, (1 - dp) * 4 + r2
    pieces_here = (piece, p_y, p_x, p_xy)
    pieces_mate = (dp * 4 + r1, dp * 4 + 3 - r, (1 - dp) * 4 + r1, (1 - dp) * 4 + 3 - r)

    def w_at(p):
        return webuf.at[rows(p, w_rows)]

    def wo_at(p):
        return wo_buf.at[pl.ds(1, 3), rows(p, o_rows)]

    loads = [
        pltpu.make_async_copy(x_ref, xbuf.at[0], load_sem.at[0]),
        pltpu.make_async_copy(w_ref, wbuf, load_sem.at[1]),
        pltpu.make_async_copy(wo_ref, wo_buf.at[0], load_sem.at[2]),
    ]
    for c in loads:
        c.start()

    barrier = pltpu.get_barrier_semaphore()
    peers = over_z[1:] + (over_core, over_y, over_x)
    for peer in peers:
        pl.semaphore_signal(barrier, inc=1, device_id=peer, device_id_type=MESH)
    pl.semaphore_wait(barrier, len(peers))

    @pl.when(is_edge)
    def _():
        send(WZ, w_ref.at[rows(piece, w_rows)], w_at(piece), over_z[1])
        for h in range(2):
            send(E1 + h, x_ref.at[x_half[h]], xbuf.at[1, x_half[h]], over_z[1])

    @pl.when(is_inner)
    def _():
        send(C1, x_ref, xbuf.at[2], over_z[3])

    def project(slot, w, col0, dst):
        def step(n, carry):
            col = pl.multiple_of(n * HD, HD)
            res = jnp.dot(xbuf[slot], w[:, pl.ds(col0 + col, HD)], preferred_element_type=jnp.float32)
            dst[:, pl.ds(col, HD)] = res.astype(jnp.bfloat16)
            return carry

        lax.fori_loop(0, 2, step, 0)

    def kv_slot(j, rr):
        return kv_buf.at[half_id(t_of[j], rr)]

    def spread(j):
        send(SP_Y + j, kv_slot(j, r), kv_slot(j, r), over_y)
        send(SP_OWN + j, kv_slot(j, r), kv_slot(j, r), over_core)

    def spread_on(j):
        arrived(SP_Y + j, kv_slot(j, r2))
        send(SP_FAR + j, kv_slot(j, r2), kv_slot(j, r2), over_core)

    def spread_wait(j):
        arrived(SP_OWN + j, kv_slot(j, r1))
        arrived(SP_FAR + j, kv_slot(j, 3 - r))

    def own_heads(j):
        project(j, wbuf, 0, kv_slot(j, r))
        project(j, wbuf, HW, q_buf.at[t_of[j]])

    def edge_heads(i, j):
        project(j, webuf, 0, made.at[i, 0])
        project(j, webuf, HW, made.at[i, 1])

    def ship(i, j):
        t = t_of[j]
        send(SHIP_KV + i, made.at[i, 0], kv_buf.at[half_id(t, r)], over_z[1])
        send(SHIP_Q + i, made.at[i, 1], q_buf.at[t], over_z[1])

    loads[0].wait()
    loads[1].wait()
    own_heads(0)
    spread(0)
    m_ref[...] = jnp.full(m_ref.shape, NEG_BIG, jnp.float32)
    l_ref[...] = jnp.zeros(l_ref.shape, jnp.float32)
    acc_ref[...] = jnp.zeros(acc_ref.shape, jnp.float32)

    @pl.when(is_inner)
    def _():
        arrived(WZ, w_at(piece))
        send(WX, w_at(piece), w_at(piece), over_x)
        send(WY, w_at(piece), w_at(piece), over_y)
        send(WC, w_at(piece), w_at(piece), over_core)
        arrived(WY, w_at(p_y))
        send(WXY, w_at(p_y), w_at(p_y), over_x)
        send(WC + 1, w_at(p_y), w_at(p_y), over_core)
        arrived(WX, w_at(p_x))
        send(WC + 2, w_at(p_x), w_at(p_x), over_core)
        arrived(E1, xbuf.at[1, x_half[0]])
        send(C2, xbuf.at[1, x_half[0]], xbuf.at[3, x_half[0]], over_z[3])
        arrived(WXY, w_at(p_xy))
        send(WC + 3, w_at(p_xy), w_at(p_xy), over_core)
        for i in range(4):
            arrived(WC + i, w_at(pieces_mate[i]))
        edge_heads(0, 0)
        ship(0, 0)
        arrived(C1, xbuf.at[2])
        own_heads(2)
        spread(2)
        arrived(E1 + 1, xbuf.at[1, x_half[1]])
        send(C2 + 1, xbuf.at[1, x_half[1]], xbuf.at[3, x_half[1]], over_z[3])
        edge_heads(1, 2)
        ship(1, 2)
        own_heads(1)
        spread(1)

    @pl.when(is_edge)
    def _():
        arrived(SHIP_KV, kv_slot(1, r))
        spread(1)
        arrived(SHIP_KV + 1, kv_slot(2, r))
        spread(2)
        arrived(SHIP_Q, q_buf.at[t_of[1]])
        arrived(SHIP_Q + 1, q_buf.at[t_of[2]])

    scale = LOG2E * HD ** -0.5

    def tile(t, g, gap, masked):
        k_blk = kv_buf[g, :, 0:HD]
        v_blk = kv_buf[g, :, HD:HW]
        for sub in range(2 * HB // SUB):
            head, off = divmod(sub * SUB, HB)
            rs = pl.ds(sub * SUB, SUB)
            q_sub = q_buf[t, pl.ds(off, SUB), head * HD:(head + 1) * HD]
            s = lax.dot_general(q_sub, k_blk, (((1,), (1,)), ((), ())), preferred_element_type=jnp.float32)
            if masked:
                dist = gap * HB + off + lax.broadcasted_iota(jnp.int32, (SUB, HB), 0) - lax.broadcasted_iota(jnp.int32, (SUB, HB), 1)
                s = jnp.where((dist >= 0) & (dist < WINDOW), s, -jnp.inf)
            m_old = m_ref[t, rs, :]
            m_new = jnp.maximum(m_old, jnp.max(s, axis=1, keepdims=True))
            alpha = jnp.exp2((m_old - m_new) * scale)
            p = jnp.exp2((s - m_new[:, 0:1]) * scale)
            l_new = p[:, 0:128] + p[:, 128:256] + p[:, 256:384] + p[:, 384:512]
            pv = jnp.dot(p.astype(jnp.bfloat16), v_blk, preferred_element_type=jnp.float32)
            m_ref[t, rs, :] = m_new
            l_ref[t, rs, :] = l_ref[t, rs, :] * alpha + l_new
            acc_ref[t, rs, :] = acc_ref[t, rs, :] * jnp.concatenate([alpha, alpha], axis=1) + pv

    def pick(j):
        return (j == 0) * t_of[0] + (j == 1) * t_of[1] + (j == 2) * t_of[2] + (j == 3) * t_of[3]

    def attend(n, combo):
        def step(i, carry):
            jq, jk = combo(i // 4)
            t = pick(jq)
            g = half_id(pick(jk), i % 4)
            gap = half_id(t, r) - g

            @pl.when((gap > 0) & (gap < 8))
            def _():
                tile(t, g, gap, False)

            @pl.when((gap == 0) | (gap == 8))
            def _():
                tile(t, g, gap, True)

            return carry

        lax.fori_loop(0, 4 * n, step, 0)

    def finish(t):
        for sub in range(2 * HB // SUB):
            head, off = divmod(sub * SUB, HB)
            rs = pl.ds(sub * SUB, SUB)
            total = jnp.sum(l_ref[t, rs, :], axis=1, keepdims=True)
            o_buf[t, pl.ds(off, SUB), head * HD:(head + 1) * HD] = (acc_ref[t, rs, :] / total).astype(jnp.bfloat16)

    for j in range(3):
        spread_on(j)
    spread_wait(0)
    spread_wait(1)
    attend(4, lambda i: (i % 2, i // 2))

    for k in range(1, 4):
        send(OZ + k, wo_ref.at[rows(piece, o_rows)], wo_buf.at[k, rows(piece, o_rows)], over_z[k])

    @pl.when(is_inner)
    def _():
        for h in range(2):
            arrived(C2 + h, xbuf.at[3, x_half[h]])
        project(3, webuf, 0, made.at[2, 0])
        project(3, wbuf, 0, kv_slot(3, r))
        send(SHIP_KV + 2, made.at[2, 0], kv_slot(3, r), over_z[1])
        spread(3)
        project(3, webuf, HW, made.at[2, 1])
        project(3, wbuf, HW, q_buf.at[t_of[3]])
        send(SHIP_Q + 2, made.at[2, 1], q_buf.at[t_of[3]], over_z[1])

    @pl.when(is_edge)
    def _():
        arrived(SHIP_KV + 2, kv_slot(3, r))
        spread(3)

    spread_wait(2)
    attend(5, lambda i: (jnp.minimum(i, 2), jnp.where(i < 3, 2, i - 3)))

    for k in range(1, 4):
        arrived(OZ + k, wo_buf.at[k, rows(piece, o_rows)])
    send(OX, wo_at(piece), wo_at(piece), over_x)
    send(OY, wo_at(piece), wo_at(piece), over_y)
    send(OC, wo_at(piece), wo_at(piece), over_core)

    spread_on(3)

    @pl.when(is_edge)
    def _():
        arrived(SHIP_Q + 2, q_buf.at[t_of[3]])

    spread_wait(3)
    attend(5, lambda i: (jnp.where(i < 4, 3, 2), jnp.minimum(i, 3)))
    for k in range(2, 4):
        finish(z_by[k])
    for k in range(2, 4):
        send(HOME + k, o_buf.at[z_by[k]], o_recv.at[k - 1], over_z[k])
    arrived(OY, wo_at(p_y))
    send(OXY, wo_at(p_y), wo_at(p_y), over_x)
    send(OC + 1, wo_at(p_y), wo_at(p_y), over_core)
    arrived(OX, wo_at(p_x))
    send(OC + 2, wo_at(p_x), wo_at(p_x), over_core)
    attend(2, lambda i: (1 - i, 3))
    finish(z_by[1])
    finish(z)
    send(HOME + 1, o_buf.at[z_by[1]], o_recv.at[0], over_z[1])
    arrived(OXY, wo_at(p_xy))
    send(OC + 3, wo_at(p_xy), wo_at(p_xy), over_core)
    for i in range(4):
        arrived(OC + i, wo_at(pieces_mate[i]))
    loads[2].wait()
    for k in range(1, 4):
        arrived(HOME + k, o_recv.at[k - 1])

    def out_step(n, carry):
        cols = rows(n, HD)
        total = jnp.dot(o_buf[z], wo_buf[0, :, cols], preferred_element_type=jnp.float32)
        for k in range(1, 4):
            total = total + jnp.dot(o_recv[k - 1], wo_buf[k, :, cols], preferred_element_type=jnp.float32)
        y_ref[:, cols] = total.astype(jnp.bfloat16)
        return carry

    lax.fori_loop(0, d_model // HD, out_step, 0)

    @pl.when(is_edge)
    def _():
        sent(WZ, w_at(piece))
        for h in range(2):
            sent(E1 + h, xbuf.at[1, x_half[h]])

    @pl.when(is_inner)
    def _():
        sent(C1, xbuf.at[2])
        for h in range(2):
            sent(C2 + h, xbuf.at[3, x_half[h]])
        for idx in (WY, WX, WXY, WC, WC + 1, WC + 2, WC + 3):
            sent(idx, w_at(piece))
        for i in range(3):
            sent(SHIP_KV + i, made.at[i, 0])
            sent(SHIP_Q + i, made.at[i, 1])

    for j in range(4):
        for base in (SP_Y, SP_OWN, SP_FAR):
            sent(base + j, kv_slot(j, r))
    for k in range(1, 4):
        sent(OZ + k, wo_buf.at[k, rows(piece, o_rows)])
        sent(HOME + k, o_recv.at[k - 1])
    for idx in (OY, OX, OXY, OC, OC + 1, OC + 2, OC + 3):
        sent(idx, wo_at(piece))


def solution(mesh):
    def local_attn(x, w_query, w_key, w_value, w_out):
        d_model = x.shape[1]
        w_own = jnp.concatenate([w_key.reshape(d_model, HD), w_value.reshape(d_model, HD), w_query.reshape(d_model, HW)], axis=1)
        bf16, f32 = jnp.bfloat16, jnp.float32
        return pl.pallas_call(
            sublayer_kernel,
            out_shape=jax.ShapeDtypeStruct((HB, d_model), bf16),
            in_specs=[pl.BlockSpec(memory_space=pl.ANY)] * 3,
            out_specs=pl.BlockSpec(memory_space=pltpu.VMEM),
            scratch_shapes=[
                pltpu.VMEM((4, HB, d_model), bf16),
                pltpu.VMEM((d_model, 2 * HW), bf16),
                pltpu.VMEM((d_model, 2 * HW), bf16),
                pltpu.VMEM((4, HB, HW), bf16),
                pltpu.VMEM((16, HB, HW), bf16),
                pltpu.VMEM((3, 2, HB, HW), bf16),
                pltpu.VMEM((4, 2 * HB, 128), f32),
                pltpu.VMEM((4, 2 * HB, 128), f32),
                pltpu.VMEM((4, 2 * HB, HD), f32),
                pltpu.VMEM((4, HB, HW), bf16),
                pltpu.VMEM((3, HB, HW), bf16),
                pltpu.VMEM((4, HW, d_model), bf16),
                pltpu.SemaphoreType.DMA((N_TX,)),
                pltpu.SemaphoreType.DMA((N_TX,)),
                pltpu.SemaphoreType.DMA((3,)),
            ],
            compiler_params=pltpu.CompilerParams(collective_id=0, has_side_effects=True, vmem_limit_bytes=67043328),
            cost_estimate=pl.CostEstimate(flops=40_000_000_000, bytes_accessed=20_000_000, transcendentals=18_000_000),
            name="sublayer",
        )(x, w_own, w_out.reshape(HW, d_model))

    return jax.shard_map(local_attn, mesh=mesh, in_specs=(P(("dp", "sp", "tp"), None), P(None, "tp", None), P(None, "tp", None), P(None, "tp", None), P("tp", None, None)), out_specs=P(("dp", "sp", "tp"), None), check_vma=False)
```

```python
import functools

import jax
import jax.numpy as jnp
from jax import lax
from jax.experimental import pallas as pl
from jax.experimental.pallas import tpu as pltpu
from jax.sharding import PartitionSpec as P

LOG2E = 1.4426950408889634
WINDOW = 4096
NEG_BIG = -1e30
MESH = pl.DeviceIdType.MESH

HB = 512
HD = 256
HW = 2 * HD
SUB = 256

_COUNT = (2, 1, 2, 1, 1, 1, 1, 4, 2, 2, 2, 2, 3, 3, 3, 2, 2, 2, 1, 7, 2, 2, 7, 4)
_START = [sum(_COUNT[:i]) for i in range(len(_COUNT))]
E1, C1, C2, WZ, WY, WX, WXY, WC, SHIP_KV, SHIP_Q, SHIPD_KV, SHIPD_Q, SP_Y, SP_OWN, SP_FAR, SPD_Y, SPD_OWN, SPD_FAR, OZ, ONE, OCROSS, OEDGE, TWO, HOME = _START
N_TX = sum(_COUNT)


def sublayer_kernel(x_ref, wk_ref, wv_ref, wq_ref, wo_ref, y_ref, y32, xbuf, wbuf, webuf, q_buf, kv_buf, made, m_ref, l_ref, acc_ref, o_buf, o_recv, wo_buf, send_sem, recv_sem, load_sem):
    z, r, dp = lax.axis_index("tp"), lax.axis_index("sp"), lax.axis_index("dp")
    z_by = (z, z + 1 - 2 * (z % 2), z + 2 - 4 * (z // 2), 3 - z)
    r1, r2 = r + 1 - 2 * (r % 2), r + 2 - 4 * (r // 2)
    inner = ((z + 1) // 2) % 2
    is_inner, is_edge = inner == 1, inner == 0
    d_model = xbuf.shape[2]
    w_rows, o_rows = d_model // 8, HW // 8

    t_c = inner * (3 - z) + (1 - inner) * z_by[2]
    t_d = inner * z_by[2] + (1 - inner) * (3 - z)
    t_of = (z, z_by[1], t_c, t_d)

    def half_id(t, rr):
        return t + 2 * rr + (t // 2) * (12 - 4 * rr)

    def to(**axes):
        return axes

    over_z = tuple(to(tp=z_by[k]) for k in range(4))
    over_core, over_y, over_x = to(sp=r1), to(sp=r2), to(dp=1 - dp)

    def tx(idx, src, dst, device):
        return pltpu.make_async_remote_copy(src_ref=src, dst_ref=dst, send_sem=send_sem.at[idx], recv_sem=recv_sem.at[idx], device_id=device, device_id_type=MESH)

    def send(idx, src, dst, device):
        tx(idx, src, dst, device).start()

    def arrived(idx, dst):
        tx(idx, dst, dst, over_core).wait_recv()

    def sent(idx, src):
        tx(idx, src, src, over_core).wait_send()

    def rows(n, size):
        return pl.ds(pl.multiple_of(n * size, size), size)

    x_half = [pl.ds(0, HB // 2), pl.ds(HB // 2, HB // 2)]
    piece = dp * 4 + r
    p_y, p_x, p_xy = dp * 4 + r2, (1 - dp) * 4 + r, (1 - dp) * 4 + r2
    pieces_here = (piece, p_y, p_x, p_xy)
    pieces_mate = (dp * 4 + r1, dp * 4 + 3 - r, (1 - dp) * 4 + r1, (1 - dp) * 4 + 3 - r)

    def w_at(p):
        return webuf.at[rows(p, w_rows)]

    def wo_at(first, n, p):
        return wo_buf.at[pl.ds(first, n), rows(p, o_rows)]

    loads = [
        pltpu.make_async_copy(wk_ref, wbuf.at[:, 0:HD], load_sem.at[0]),
        pltpu.make_async_copy(wv_ref, wbuf.at[:, HD:HW], load_sem.at[1]),
        pltpu.make_async_copy(wq_ref, wbuf.at[:, HW:2 * HW], load_sem.at[2]),
        pltpu.make_async_copy(x_ref, xbuf.at[0], load_sem.at[3]),
        pltpu.make_async_copy(wo_ref, wo_buf.at[0], load_sem.at[4]),
    ]
    for c in loads:
        c.start()

    barrier = pltpu.get_barrier_semaphore()
    peers = over_z[1:] + (over_core, over_y, over_x)
    for peer in peers:
        pl.semaphore_signal(barrier, inc=1, device_id=peer, device_id_type=MESH)
    pl.semaphore_wait(barrier, len(peers))

    @pl.when(is_inner)
    def _():
        send(C1, x_ref, xbuf.at[2], over_z[3])

    for c in loads[:3]:
        c.wait()

    def out_edge():
        send(OZ, wo_ref.at[rows(piece, o_rows)], wo_buf.at[1, rows(piece, o_rows)], over_z[1])

    @pl.when(is_edge)
    def _():
        send(WZ, wbuf.at[rows(piece, w_rows)], w_at(piece), over_z[1])
        send(E1, x_ref.at[x_half[0]], xbuf.at[1, x_half[0]], over_z[1])
        out_edge()
        send(E1 + 1, x_ref.at[x_half[1]], xbuf.at[1, x_half[1]], over_z[1])

    @pl.when(is_inner)
    def _():
        out_edge()

    def project(slot, part, w, col0, dst):
        def step(n, carry):
            col = pl.multiple_of(n * HD, HD)
            res = jnp.dot(xbuf[slot, part, :], w[:, pl.ds(col0 + col, HD)], preferred_element_type=jnp.float32)
            dst[:, pl.ds(col, HD)] = res.astype(jnp.bfloat16)
            return carry

        lax.fori_loop(0, 2, step, 0)

    whole = pl.ds(0, HB)

    def kv_slot(j, rr):
        return kv_buf.at[half_id(t_of[j], rr)]

    def kvd(h, rr):
        return kv_buf.at[half_id(t_of[3], rr), x_half[h]]

    def spread(j):
        send(SP_Y + j, kv_slot(j, r), kv_slot(j, r), over_y)
        send(SP_OWN + j, kv_slot(j, r), kv_slot(j, r), over_core)

    def spread_on(j):
        arrived(SP_Y + j, kv_slot(j, r2))
        send(SP_FAR + j, kv_slot(j, r2), kv_slot(j, r2), over_core)

    def spread_wait(j):
        arrived(SP_OWN + j, kv_slot(j, r1))
        arrived(SP_FAR + j, kv_slot(j, 3 - r))

    def spread_last(h):
        send(SPD_Y + h, kvd(h, r), kvd(h, r), over_y)
        send(SPD_OWN + h, kvd(h, r), kvd(h, r), over_core)

    def spread_last_on(h):
        arrived(SPD_Y + h, kvd(h, r2))
        send(SPD_FAR + h, kvd(h, r2), kvd(h, r2), over_core)

    def spread_last_wait(h):
        arrived(SPD_OWN + h, kvd(h, r1))
        arrived(SPD_FAR + h, kvd(h, 3 - r))

    def own_heads(j):
        project(j, whole, wbuf, 0, kv_slot(j, r))
        project(j, whole, wbuf, HW, q_buf.at[t_of[j]])

    def edge_heads(i, j):
        t = t_of[j]
        project(j, whole, webuf, 0, made.at[i, 0])
        project(j, whole, webuf, HW, made.at[i, 1])
        send(SHIP_KV + i, made.at[i, 0], kv_buf.at[half_id(t, r)], over_z[1])
        send(SHIP_Q + i, made.at[i, 1], q_buf.at[t], over_z[1])

    def last_rows(h):
        part = x_half[h]
        arrived(C2 + h, xbuf.at[3, part])
        project(3, part, webuf, 0, made.at[2, 0, part])
        project(3, part, wbuf, 0, kvd(h, r))
        send(SHIPD_KV + h, made.at[2, 0, part], kvd(h, r), over_z[1])
        spread_last(h)
        project(3, part, webuf, HW, made.at[2, 1, part])
        project(3, part, wbuf, HW, q_buf.at[t_of[3], part])
        send(SHIPD_Q + h, made.at[2, 1, part], q_buf.at[t_of[3], part], over_z[1])

    def out_hop(base, first, n):
        send(base, wo_at(first, n, piece), wo_at(first, n, piece), over_x)
        send(base + 1, wo_at(first, n, piece), wo_at(first, n, piece), over_y)
        send(base + 3, wo_at(first, n, piece), wo_at(first, n, piece), over_core)

    def out_hop2(base, first, n):
        arrived(base + 1, wo_at(first, n, p_y))
        send(base + 2, wo_at(first, n, p_y), wo_at(first, n, p_y), over_x)
        send(base + 4, wo_at(first, n, p_y), wo_at(first, n, p_y), over_core)
        arrived(base, wo_at(first, n, p_x))
        send(base + 5, wo_at(first, n, p_x), wo_at(first, n, p_x), over_core)

    def out_hop3(base, first, n):
        arrived(base + 2, wo_at(first, n, p_xy))
        send(base + 6, wo_at(first, n, p_xy), wo_at(first, n, p_xy), over_core)

    def out_wait(base, first, n):
        for i in range(4):
            arrived(base + 3 + i, wo_at(first, n, pieces_mate[i]))

    loads[3].wait()
    own_heads(0)
    spread(0)
    m_ref[...] = jnp.full(m_ref.shape, NEG_BIG, jnp.float32)
    l_ref[...] = jnp.zeros(l_ref.shape, jnp.float32)
    acc_ref[...] = jnp.zeros(acc_ref.shape, jnp.float32)

    @pl.when(is_inner)
    def _():
        arrived(WZ, w_at(piece))
        send(WX, w_at(piece), w_at(piece), over_x)
        send(WY, w_at(piece), w_at(piece), over_y)
        send(WC, w_at(piece), w_at(piece), over_core)
        arrived(WY, w_at(p_y))
        send(WXY, w_at(p_y), w_at(p_y), over_x)
        send(WC + 1, w_at(p_y), w_at(p_y), over_core)
        arrived(WX, w_at(p_x))
        send(WC + 2, w_at(p_x), w_at(p_x), over_core)
        spread_on(0)
        arrived(E1, xbuf.at[1, x_half[0]])
        send(C2, xbuf.at[1, x_half[0]], xbuf.at[3, x_half[0]], over_z[3])
        arrived(WXY, w_at(p_xy))
        send(WC + 3, w_at(p_xy), w_at(p_xy), over_core)
        for i in range(4):
            arrived(WC + i, w_at(pieces_mate[i]))
        edge_heads(0, 0)
        arrived(OZ, wo_buf.at[1, rows(piece, o_rows)])
        out_hop(ONE, 1, 1)
        arrived(C1, xbuf.at[2])
        own_heads(2)
        spread(2)
        arrived(E1 + 1, xbuf.at[1, x_half[1]])
        send(C2 + 1, xbuf.at[1, x_half[1]], xbuf.at[3, x_half[1]], over_z[3])
        send(OCROSS, wo_ref.at[rows(piece, o_rows)], wo_buf.at[3, rows(piece, o_rows)], over_z[3])
        send(OCROSS + 1, wo_buf.at[1, rows(piece, o_rows)], wo_buf.at[2, rows(piece, o_rows)], over_z[3])
        edge_heads(1, 2)
        own_heads(1)
        spread(1)
        spread_on(2)
        last_rows(0)
        spread_on(1)

    @pl.when(is_edge)
    def _():
        arrived(OZ, wo_buf.at[1, rows(piece, o_rows)])
        out_hop(ONE, 1, 1)
        spread_on(0)
        arrived(SHIP_KV, kv_slot(1, r))
        spread(1)
        arrived(SHIP_Q, q_buf.at[t_of[1]])
        spread_on(1)
        arrived(SHIP_KV + 1, kv_slot(2, r))
        spread(2)

    scale = LOG2E * HD ** -0.5

    def tile(t, g, gap, masked):
        k_blk = kv_buf[g, :, 0:HD]
        v_blk = kv_buf[g, :, HD:HW]
        n_sub = 2 * HB // SUB

        def scores(sub):
            head, off = divmod(sub * SUB, HB)
            q_sub = q_buf[t, pl.ds(off, SUB), head * HD:(head + 1) * HD]
            return lax.dot_general(q_sub, k_blk, (((1,), (1,)), ((), ())), preferred_element_type=jnp.float32)

        ahead = scores(0)
        for sub in range(n_sub):
            off = sub * SUB % HB
            rs = pl.ds(sub * SUB, SUB)
            s = ahead
            if sub + 1 < n_sub:
                ahead = scores(sub + 1)
            if masked:
                dist = gap * HB + off + lax.broadcasted_iota(jnp.int32, (SUB, HB), 0) - lax.broadcasted_iota(jnp.int32, (SUB, HB), 1)
                s = jnp.where((dist >= 0) & (dist < WINDOW), s, -jnp.inf)
            m_old = m_ref[t, rs, :]
            m_new = jnp.maximum(m_old, jnp.max(s, axis=1, keepdims=True))
            alpha = jnp.exp2((m_old - m_new) * scale)
            p = jnp.exp2((s - jnp.concatenate([m_new] * 4, axis=1)) * scale)
            l_new = p[:, 0:128] + p[:, 128:256] + p[:, 256:384] + p[:, 384:512]
            pv = jnp.dot(p.astype(jnp.bfloat16), v_blk, preferred_element_type=jnp.float32)
            m_ref[t, rs, :] = m_new
            l_ref[t, rs, :] = l_ref[t, rs, :] * alpha + l_new
            acc_ref[t, rs, :] = acc_ref[t, rs, :] * jnp.concatenate([alpha, alpha], axis=1) + pv

    def pick(j):
        return (j == 0) * t_of[0] + (j == 1) * t_of[1] + (j == 2) * t_of[2] + (j == 3) * t_of[3]

    def attend(n, combo):
        def step(i, carry):
            jq, jk = combo(i // 4)
            t = pick(jq)
            g = half_id(pick(jk), i % 4)
            gap = half_id(t, r) - g

            @pl.when((gap > 0) & (gap < 8))
            def _():
                tile(t, g, gap, False)

            @pl.when((gap == 0) | (gap == 8))
            def _():
                tile(t, g, gap, True)

            return carry

        lax.fori_loop(0, 4 * n, step, 0)

    def finish(t):
        for sub in range(2 * HB // SUB):
            head, off = divmod(sub * SUB, HB)
            rs = pl.ds(sub * SUB, SUB)
            total = jnp.sum(l_ref[t, rs, :], axis=1, keepdims=True)
            o_buf[t, pl.ds(off, SUB), head * HD:(head + 1) * HD] = (acc_ref[t, rs, :] / total).astype(jnp.bfloat16)

    spread_wait(0)
    spread_wait(1)
    attend(4 * (1 - inner), lambda i: (i % 2, i // 2))

    @pl.when(is_edge)
    def _():
        arrived(SHIPD_KV, kvd(0, r))
        spread_last(0)
        spread_on(2)
        arrived(SHIP_Q + 1, q_buf.at[t_of[2]])

    out_hop2(ONE, 1, 1)
    spread_wait(2)
    attend(3, lambda i: (2, i))
    spread_last_on(0)

    @pl.when(is_inner)
    def _():
        last_rows(1)

    @pl.when(is_edge)
    def _():
        arrived(SHIPD_KV + 1, kvd(1, r))
        spread_last(1)
        for h in range(2):
            arrived(SHIPD_Q + h, q_buf.at[t_of[3], x_half[h]])

    out_hop3(ONE, 1, 1)
    attend(3, lambda i: (3, i))
    spread_last_on(1)
    for h in range(2):
        spread_last_wait(h)
    attend(1, lambda i: (2, 3))
    finish(t_c)

    def home(t, by_inner, by_edge):
        @pl.when(is_inner)
        def _():
            send(HOME + by_inner, o_buf.at[t], o_recv.at[by_inner - 1], over_z[by_inner])

        @pl.when(is_edge)
        def _():
            send(HOME + by_edge, o_buf.at[t], o_recv.at[by_edge - 1], over_z[by_edge])

    home(t_c, 3, 2)

    @pl.when(is_inner)
    def _():
        for i in range(2):
            arrived(OCROSS + i, wo_buf.at[3 - i, rows(piece, o_rows)])
            send(OEDGE + i, wo_buf.at[3 - i, rows(piece, o_rows)], wo_buf.at[2 + i, rows(piece, o_rows)], over_z[1])

    attend(1, lambda i: (3, 3))
    finish(t_d)
    home(t_d, 2, 3)

    @pl.when(is_edge)
    def _():
        for i in range(2):
            arrived(OEDGE + i, wo_buf.at[2 + i, rows(piece, o_rows)])

    out_hop(TWO, 2, 2)
    attend(4 + 4 * inner, lambda i: (i % 2, (i // 2 + 2) % 4))
    finish(z_by[1])
    finish(z)
    send(HOME + 1, o_buf.at[z_by[1]], o_recv.at[0], over_z[1])
    out_hop2(TWO, 2, 2)
    out_wait(ONE, 1, 1)
    loads[4].wait()
    arrived(HOME + 1, o_recv.at[0])

    def out_near(n, carry):
        cols = rows(n, HD)
        near = jnp.dot(o_buf[z], wo_buf[0, :, cols], preferred_element_type=jnp.float32)
        y32[:, cols] = near + jnp.dot(o_recv[0], wo_buf[1, :, cols], preferred_element_type=jnp.float32)
        return carry

    lax.fori_loop(0, d_model // HD, out_near, 0)
    out_hop3(TWO, 2, 2)
    out_wait(TWO, 2, 2)
    for k in range(2, 4):
        arrived(HOME + k, o_recv.at[k - 1])

    def out_far(n, carry):
        cols = rows(n, HD)
        far = jnp.dot(o_recv[1], wo_buf[2, :, cols], preferred_element_type=jnp.float32)
        far = far + jnp.dot(o_recv[2], wo_buf[3, :, cols], preferred_element_type=jnp.float32)
        y_ref[:, cols] = (y32[:, cols] + far).astype(jnp.bfloat16)
        return carry

    lax.fori_loop(0, d_model // HD, out_far, 0)

    @pl.when(is_edge)
    def _():
        sent(WZ, w_at(piece))
        for h in range(2):
            sent(E1 + h, xbuf.at[1, x_half[h]])

    @pl.when(is_inner)
    def _():
        sent(C1, xbuf.at[2])
        for h in range(2):
            sent(C2 + h, xbuf.at[3, x_half[h]])
            sent(SHIPD_KV + h, made.at[2, 0, x_half[h]])
            sent(SHIPD_Q + h, made.at[2, 1, x_half[h]])
            sent(SHIP_KV + h, made.at[h, 0])
            sent(SHIP_Q + h, made.at[h, 1])
            sent(OCROSS + h, wo_buf.at[2 + h, rows(piece, o_rows)])
            sent(OEDGE + h, wo_buf.at[2 + h, rows(piece, o_rows)])
        for idx in (WY, WX, WXY, WC, WC + 1, WC + 2, WC + 3):
            sent(idx, w_at(piece))

    for j in range(3):
        for base in (SP_Y, SP_OWN, SP_FAR):
            sent(base + j, kv_slot(j, r))
    for h in range(2):
        for base in (SPD_Y, SPD_OWN, SPD_FAR):
            sent(base + h, kvd(h, r))
    sent(OZ, wo_buf.at[1, rows(piece, o_rows)])
    for i in range(7):
        sent(ONE + i, wo_at(1, 1, piece))
        sent(TWO + i, wo_at(2, 2, piece))
    for k in range(1, 4):
        sent(HOME + k, o_recv.at[k - 1])


def solution(mesh):
    def local_attn(x, w_query, w_key, w_value, w_out):
        d_model = x.shape[1]
        bf16, f32 = jnp.bfloat16, jnp.float32
        return pl.pallas_call(
            sublayer_kernel,
            out_shape=jax.ShapeDtypeStruct((HB, d_model), bf16),
            in_specs=[pl.BlockSpec(memory_space=pl.ANY)] * 5,
            out_specs=pl.BlockSpec(memory_space=pltpu.VMEM),
            scratch_shapes=[
                pltpu.VMEM((HB, d_model), f32),
                pltpu.VMEM((4, HB, d_model), bf16),
                pltpu.VMEM((d_model, 2 * HW), bf16),
                pltpu.VMEM((d_model, 2 * HW), bf16),
                pltpu.VMEM((4, HB, HW), bf16),
                pltpu.VMEM((16, HB, HW), bf16),
                pltpu.VMEM((3, 2, HB, HW), bf16),
                pltpu.VMEM((4, 2 * HB, 128), f32),
                pltpu.VMEM((4, 2 * HB, 128), f32),
                pltpu.VMEM((4, 2 * HB, HD), f32),
                pltpu.VMEM((4, HB, HW), bf16),
                pltpu.VMEM((3, HB, HW), bf16),
                pltpu.VMEM((4, HW, d_model), bf16),
                pltpu.SemaphoreType.DMA((N_TX,)),
                pltpu.SemaphoreType.DMA((N_TX,)),
                pltpu.SemaphoreType.DMA((5,)),
            ],
            compiler_params=pltpu.CompilerParams(collective_id=0, has_side_effects=True, vmem_limit_bytes=67043328),
            cost_estimate=pl.CostEstimate(flops=40_000_000_000, bytes_accessed=20_000_000, transcendentals=18_000_000),
            name="sublayer",
        )(x, w_key.reshape(d_model, HD), w_value.reshape(d_model, HD), w_query.reshape(d_model, HW), w_out.reshape(HW, d_model))

    return jax.shard_map(local_attn, mesh=mesh, in_specs=(P(("dp", "sp", "tp"), None), P(None, "tp", None), P(None, "tp", None), P(None, "tp", None), P("tp", None, None)), out_specs=P(("dp", "sp", "tp"), None), check_vma=False)
```

```python
import functools

import jax
import jax.numpy as jnp
from jax import lax
from jax.experimental import pallas as pl
from jax.experimental.pallas import tpu as pltpu
from jax.sharding import PartitionSpec as P

LOG2E = 1.4426950408889634
WINDOW = 4096
NEG_BIG = -1e30
MESH = pl.DeviceIdType.MESH

HB = 512
HD = 256
HW = 2 * HD
SUB = 256

_COUNT = (2, 1, 3, 1, 1, 1, 1, 4, 2, 2, 3, 3, 3, 3, 3, 3, 3, 3, 1, 7, 2, 2, 7, 4)
_START = [sum(_COUNT[:i]) for i in range(len(_COUNT))]
E1, C1, C2, WZ, WY, WX, WXY, WC, SHIP_KV, SHIP_Q, SHIPD_KV, SHIPD_Q, SP_Y, SP_OWN, SP_FAR, SPD_Y, SPD_OWN, SPD_FAR, OZ, ONE, OCROSS, OEDGE, TWO, HOME = _START
N_TX = sum(_COUNT)


def sublayer_kernel(x_ref, wk_ref, wv_ref, wq_ref, wo_ref, y_ref, y32, xbuf, wbuf, webuf, q_buf, kv_buf, made, m_ref, l_ref, acc_ref, o_buf, o_recv, wo_buf, send_sem, recv_sem, load_sem):
    z, r, dp = lax.axis_index("tp"), lax.axis_index("sp"), lax.axis_index("dp")
    z_by = (z, z + 1 - 2 * (z % 2), z + 2 - 4 * (z // 2), 3 - z)
    r1, r2 = r + 1 - 2 * (r % 2), r + 2 - 4 * (r // 2)
    inner = ((z + 1) // 2) % 2
    is_inner, is_edge = inner == 1, inner == 0
    d_model = xbuf.shape[2]
    w_rows, o_rows = d_model // 8, HW // 8

    t_c = inner * (3 - z) + (1 - inner) * z_by[2]
    t_d = inner * z_by[2] + (1 - inner) * (3 - z)
    t_of = (z, z_by[1], t_c, t_d)

    def half_id(t, rr):
        return t + 2 * rr + (t // 2) * (12 - 4 * rr)

    def to(**axes):
        return axes

    over_z = tuple(to(tp=z_by[k]) for k in range(4))
    over_core, over_y, over_x = to(sp=r1), to(sp=r2), to(dp=1 - dp)

    def tx(idx, src, dst, device):
        return pltpu.make_async_remote_copy(src_ref=src, dst_ref=dst, send_sem=send_sem.at[idx], recv_sem=recv_sem.at[idx], device_id=device, device_id_type=MESH)

    def send(idx, src, dst, device):
        tx(idx, src, dst, device).start()

    def arrived(idx, dst):
        tx(idx, dst, dst, over_core).wait_recv()

    def sent(idx, src):
        tx(idx, src, src, over_core).wait_send()

    def rows(n, size):
        return pl.ds(pl.multiple_of(n * size, size), size)

    x_half = [pl.ds(0, HB // 2), pl.ds(HB // 2, HB // 2)]
    x_part = [pl.ds(0, HB // 2), pl.ds(HB // 2, HB // 4), pl.ds(3 * HB // 4, HB // 4)]
    piece = dp * 4 + r
    p_y, p_x, p_xy = dp * 4 + r2, (1 - dp) * 4 + r, (1 - dp) * 4 + r2
    pieces_here = (piece, p_y, p_x, p_xy)
    pieces_mate = (dp * 4 + r1, dp * 4 + 3 - r, (1 - dp) * 4 + r1, (1 - dp) * 4 + 3 - r)

    def w_at(p):
        return webuf.at[rows(p, w_rows)]

    def wo_at(first, n, p):
        return wo_buf.at[pl.ds(first, n), rows(p, o_rows)]

    loads = [
        pltpu.make_async_copy(wk_ref, wbuf.at[:, 0:HD], load_sem.at[0]),
        pltpu.make_async_copy(wv_ref, wbuf.at[:, HD:HW], load_sem.at[1]),
        pltpu.make_async_copy(wq_ref, wbuf.at[:, HW:2 * HW], load_sem.at[2]),
        pltpu.make_async_copy(x_ref, xbuf.at[0], load_sem.at[3]),
        pltpu.make_async_copy(wo_ref, wo_buf.at[0], load_sem.at[4]),
    ]
    for c in loads:
        c.start()

    barrier = pltpu.get_barrier_semaphore()
    peers = over_z[1:] + (over_core, over_y, over_x)
    for peer in peers:
        pl.semaphore_signal(barrier, inc=1, device_id=peer, device_id_type=MESH)
    pl.semaphore_wait(barrier, len(peers))

    @pl.when(is_inner)
    def _():
        send(C1, x_ref, xbuf.at[2], over_z[3])

    for c in loads[:3]:
        c.wait()

    def out_edge():
        send(OZ, wo_ref.at[rows(piece, o_rows)], wo_buf.at[1, rows(piece, o_rows)], over_z[1])

    @pl.when(is_edge)
    def _():
        send(WZ, wbuf.at[rows(piece, w_rows)], w_at(piece), over_z[1])
        send(E1, x_ref.at[x_half[0]], xbuf.at[1, x_half[0]], over_z[1])
        out_edge()
        send(E1 + 1, x_ref.at[x_half[1]], xbuf.at[1, x_half[1]], over_z[1])

    @pl.when(is_inner)
    def _():
        out_edge()

    def project(slot, part, w, col0, dst):
        def step(n, carry):
            col = pl.multiple_of(n * HD, HD)
            res = jnp.dot(xbuf[slot, part, :], w[:, pl.ds(col0 + col, HD)], preferred_element_type=jnp.float32)
            dst[:, pl.ds(col, HD)] = res.astype(jnp.bfloat16)
            return carry

        lax.fori_loop(0, 2, step, 0)

    whole = pl.ds(0, HB)

    def kv_slot(j, rr):
        return kv_buf.at[half_id(t_of[j], rr)]

    def kvd(h, rr):
        return kv_buf.at[half_id(t_of[3], rr), x_part[h]]

    def spread(j):
        send(SP_Y + j, kv_slot(j, r), kv_slot(j, r), over_y)
        send(SP_OWN + j, kv_slot(j, r), kv_slot(j, r), over_core)

    def spread_on(j):
        arrived(SP_Y + j, kv_slot(j, r2))
        send(SP_FAR + j, kv_slot(j, r2), kv_slot(j, r2), over_core)

    def spread_wait(j):
        arrived(SP_OWN + j, kv_slot(j, r1))
        arrived(SP_FAR + j, kv_slot(j, 3 - r))

    def spread_last(h):
        send(SPD_Y + h, kvd(h, r), kvd(h, r), over_y)
        send(SPD_OWN + h, kvd(h, r), kvd(h, r), over_core)

    def spread_last_on(h):
        arrived(SPD_Y + h, kvd(h, r2))
        send(SPD_FAR + h, kvd(h, r2), kvd(h, r2), over_core)

    def spread_last_wait(h):
        arrived(SPD_OWN + h, kvd(h, r1))
        arrived(SPD_FAR + h, kvd(h, 3 - r))

    def own_heads(j):
        project(j, whole, wbuf, 0, kv_slot(j, r))
        project(j, whole, wbuf, HW, q_buf.at[t_of[j]])

    def edge_heads(i, j):
        t = t_of[j]
        project(j, whole, webuf, 0, made.at[i, 0])
        project(j, whole, webuf, HW, made.at[i, 1])
        send(SHIP_KV + i, made.at[i, 0], kv_buf.at[half_id(t, r)], over_z[1])
        send(SHIP_Q + i, made.at[i, 1], q_buf.at[t], over_z[1])

    def last_rows(h):
        part = x_part[h]
        arrived(C2 + h, xbuf.at[3, part])
        project(3, part, webuf, 0, made.at[2, 0, part])
        project(3, part, wbuf, 0, kvd(h, r))
        send(SHIPD_KV + h, made.at[2, 0, part], kvd(h, r), over_z[1])
        spread_last(h)
        project(3, part, webuf, HW, made.at[2, 1, part])
        project(3, part, wbuf, HW, q_buf.at[t_of[3], part])
        send(SHIPD_Q + h, made.at[2, 1, part], q_buf.at[t_of[3], part], over_z[1])

    def out_hop(base, first, n):
        send(base, wo_at(first, n, piece), wo_at(first, n, piece), over_x)
        send(base + 1, wo_at(first, n, piece), wo_at(first, n, piece), over_y)
        send(base + 3, wo_at(first, n, piece), wo_at(first, n, piece), over_core)

    def out_hop2(base, first, n):
        arrived(base + 1, wo_at(first, n, p_y))
        send(base + 2, wo_at(first, n, p_y), wo_at(first, n, p_y), over_x)
        send(base + 4, wo_at(first, n, p_y), wo_at(first, n, p_y), over_core)
        arrived(base, wo_at(first, n, p_x))
        send(base + 5, wo_at(first, n, p_x), wo_at(first, n, p_x), over_core)

    def out_hop3(base, first, n):
        arrived(base + 2, wo_at(first, n, p_xy))
        send(base + 6, wo_at(first, n, p_xy), wo_at(first, n, p_xy), over_core)

    def out_wait(base, first, n):
        for i in range(4):
            arrived(base + 3 + i, wo_at(first, n, pieces_mate[i]))

    loads[3].wait()
    own_heads(0)
    spread(0)
    m_ref[...] = jnp.full(m_ref.shape, NEG_BIG, jnp.float32)
    l_ref[...] = jnp.zeros(l_ref.shape, jnp.float32)
    acc_ref[...] = jnp.zeros(acc_ref.shape, jnp.float32)

    @pl.when(is_inner)
    def _():
        arrived(WZ, w_at(piece))
        send(WX, w_at(piece), w_at(piece), over_x)
        send(WY, w_at(piece), w_at(piece), over_y)
        send(WC, w_at(piece), w_at(piece), over_core)
        arrived(WY, w_at(p_y))
        send(WXY, w_at(p_y), w_at(p_y), over_x)
        send(WC + 1, w_at(p_y), w_at(p_y), over_core)
        arrived(WX, w_at(p_x))
        send(WC + 2, w_at(p_x), w_at(p_x), over_core)
        spread_on(0)
        arrived(E1, xbuf.at[1, x_half[0]])
        send(C2, xbuf.at[1, x_half[0]], xbuf.at[3, x_half[0]], over_z[3])
        arrived(WXY, w_at(p_xy))
        send(WC + 3, w_at(p_xy), w_at(p_xy), over_core)
        for i in range(4):
            arrived(WC + i, w_at(pieces_mate[i]))
        edge_heads(0, 0)
        arrived(OZ, wo_buf.at[1, rows(piece, o_rows)])
        out_hop(ONE, 1, 1)
        arrived(C1, xbuf.at[2])
        own_heads(2)
        spread(2)
        arrived(E1 + 1, xbuf.at[1, x_half[1]])
        for h in range(1, 3):
            send(C2 + h, xbuf.at[1, x_part[h]], xbuf.at[3, x_part[h]], over_z[3])
        send(OCROSS, wo_ref.at[rows(piece, o_rows)], wo_buf.at[3, rows(piece, o_rows)], over_z[3])
        send(OCROSS + 1, wo_buf.at[1, rows(piece, o_rows)], wo_buf.at[2, rows(piece, o_rows)], over_z[3])
        edge_heads(1, 2)
        own_heads(1)
        spread(1)
        spread_on(2)
        last_rows(0)
        spread_on(1)

    @pl.when(is_edge)
    def _():
        arrived(OZ, wo_buf.at[1, rows(piece, o_rows)])
        out_hop(ONE, 1, 1)
        spread_on(0)
        arrived(SHIP_KV, kv_slot(1, r))
        spread(1)
        arrived(SHIP_Q, q_buf.at[t_of[1]])
        spread_on(1)
        arrived(SHIP_KV + 1, kv_slot(2, r))
        spread(2)

    scale = LOG2E * HD ** -0.5

    def tile(t, g, gap, masked):
        k_blk = kv_buf[g, :, 0:HD]
        v_blk = kv_buf[g, :, HD:HW]
        n_sub = 2 * HB // SUB

        def scores(sub):
            head, off = divmod(sub * SUB, HB)
            q_sub = q_buf[t, pl.ds(off, SUB), head * HD:(head + 1) * HD]
            return lax.dot_general(q_sub, k_blk, (((1,), (1,)), ((), ())), preferred_element_type=jnp.float32)

        ahead = scores(0)
        for sub in range(n_sub):
            off = sub * SUB % HB
            rs = pl.ds(sub * SUB, SUB)
            s = ahead
            if sub + 1 < n_sub:
                ahead = scores(sub + 1)
            if masked:
                dist = gap * HB + off + lax.broadcasted_iota(jnp.int32, (SUB, HB), 0) - lax.broadcasted_iota(jnp.int32, (SUB, HB), 1)
                s = jnp.where((dist >= 0) & (dist < WINDOW), s, -jnp.inf)
            m_old = m_ref[t, rs, :]
            m_new = jnp.maximum(m_old, jnp.max(s, axis=1, keepdims=True))
            alpha = jnp.exp2((m_old - m_new) * scale)
            p = jnp.exp2((s - jnp.concatenate([m_new] * 4, axis=1)) * scale)
            l_new = p[:, 0:128] + p[:, 128:256] + p[:, 256:384] + p[:, 384:512]
            pv = jnp.dot(p.astype(jnp.bfloat16), v_blk, preferred_element_type=jnp.float32)
            m_ref[t, rs, :] = m_new
            l_ref[t, rs, :] = l_ref[t, rs, :] * alpha + l_new
            acc_ref[t, rs, :] = acc_ref[t, rs, :] * jnp.concatenate([alpha, alpha], axis=1) + pv

    def pick(j):
        return (j == 0) * t_of[0] + (j == 1) * t_of[1] + (j == 2) * t_of[2] + (j == 3) * t_of[3]

    def attend(n, combo):
        def step(i, carry):
            jq, jk = combo(i // 4)
            t = pick(jq)
            g = half_id(pick(jk), i % 4)
            gap = half_id(t, r) - g

            @pl.when((gap > 0) & (gap < 8))
            def _():
                tile(t, g, gap, False)

            @pl.when((gap == 0) | (gap == 8))
            def _():
                tile(t, g, gap, True)

            return carry

        lax.fori_loop(0, 4 * n, step, 0)

    def finish(t):
        for sub in range(2 * HB // SUB):
            head, off = divmod(sub * SUB, HB)
            rs = pl.ds(sub * SUB, SUB)
            total = jnp.sum(l_ref[t, rs, :], axis=1, keepdims=True)
            o_buf[t, pl.ds(off, SUB), head * HD:(head + 1) * HD] = (acc_ref[t, rs, :] / total).astype(jnp.bfloat16)

    spread_wait(0)
    spread_wait(1)
    attend(4 * (1 - inner), lambda i: (i % 2, i // 2))

    @pl.when(is_edge)
    def _():
        arrived(SHIPD_KV, kvd(0, r))
        spread_last(0)
        spread_on(2)
        arrived(SHIP_Q + 1, q_buf.at[t_of[2]])

    out_hop2(ONE, 1, 1)
    spread_wait(2)
    attend(3, lambda i: (2, i))
    spread_last_on(0)

    @pl.when(is_inner)
    def _():
        last_rows(1)
        last_rows(2)

    @pl.when(is_edge)
    def _():
        for h in range(1, 3):
            arrived(SHIPD_KV + h, kvd(h, r))
            spread_last(h)

    out_hop3(ONE, 1, 1)
    spread_last_on(1)
    attend(3 * inner, lambda i: (3, i))
    spread_last_on(2)
    for h in range(3):
        spread_last_wait(h)
    attend(1, lambda i: (2, 3))
    finish(t_c)

    def home(t, by_inner, by_edge):
        @pl.when(is_inner)
        def _():
            send(HOME + by_inner, o_buf.at[t], o_recv.at[by_inner - 1], over_z[by_inner])

        @pl.when(is_edge)
        def _():
            send(HOME + by_edge, o_buf.at[t], o_recv.at[by_edge - 1], over_z[by_edge])

    home(t_c, 3, 2)

    @pl.when(is_inner)
    def _():
        for i in range(2):
            arrived(OCROSS + i, wo_buf.at[3 - i, rows(piece, o_rows)])
            send(OEDGE + i, wo_buf.at[3 - i, rows(piece, o_rows)], wo_buf.at[2 + i, rows(piece, o_rows)], over_z[1])

    @pl.when(is_edge)
    def _():
        for h in range(3):
            arrived(SHIPD_Q + h, q_buf.at[t_of[3], x_part[h]])

    attend(4 - 3 * inner, lambda i: (3, (i + 3) % 4))
    finish(t_d)
    home(t_d, 2, 3)

    @pl.when(is_edge)
    def _():
        for i in range(2):
            arrived(OEDGE + i, wo_buf.at[2 + i, rows(piece, o_rows)])

    out_hop(TWO, 2, 2)
    attend(4 + 4 * inner, lambda i: (i % 2, (i // 2 + 2) % 4))
    finish(z_by[1])
    finish(z)
    send(HOME + 1, o_buf.at[z_by[1]], o_recv.at[0], over_z[1])
    out_hop2(TWO, 2, 2)
    out_wait(ONE, 1, 1)
    loads[4].wait()
    arrived(HOME + 1, o_recv.at[0])

    def out_near(n, carry):
        cols = rows(n, HD)
        near = jnp.dot(o_buf[z], wo_buf[0, :, cols], preferred_element_type=jnp.float32)
        y32[:, cols] = near + jnp.dot(o_recv[0], wo_buf[1, :, cols], preferred_element_type=jnp.float32)
        return carry

    lax.fori_loop(0, d_model // HD, out_near, 0)
    out_hop3(TWO, 2, 2)
    out_wait(TWO, 2, 2)
    for k in range(2, 4):
        arrived(HOME + k, o_recv.at[k - 1])

    def out_far(n, carry):
        cols = rows(n, HD)
        far = jnp.dot(o_recv[1], wo_buf[2, :, cols], preferred_element_type=jnp.float32)
        far = far + jnp.dot(o_recv[2], wo_buf[3, :, cols], preferred_element_type=jnp.float32)
        y_ref[:, cols] = (y32[:, cols] + far).astype(jnp.bfloat16)
        return carry

    lax.fori_loop(0, d_model // HD, out_far, 0)

    @pl.when(is_edge)
    def _():
        sent(WZ, w_at(piece))
        for h in range(2):
            sent(E1 + h, xbuf.at[1, x_half[h]])

    @pl.when(is_inner)
    def _():
        sent(C1, xbuf.at[2])
        for h in range(3):
            sent(C2 + h, xbuf.at[3, x_part[h]])
            sent(SHIPD_KV + h, made.at[2, 0, x_part[h]])
            sent(SHIPD_Q + h, made.at[2, 1, x_part[h]])
        for h in range(2):
            sent(SHIP_KV + h, made.at[h, 0])
            sent(SHIP_Q + h, made.at[h, 1])
            sent(OCROSS + h, wo_buf.at[2 + h, rows(piece, o_rows)])
            sent(OEDGE + h, wo_buf.at[2 + h, rows(piece, o_rows)])
        for idx in (WY, WX, WXY, WC, WC + 1, WC + 2, WC + 3):
            sent(idx, w_at(piece))

    for j in range(3):
        for base in (SP_Y, SP_OWN, SP_FAR):
            sent(base + j, kv_slot(j, r))
    for h in range(3):
        for base in (SPD_Y, SPD_OWN, SPD_FAR):
            sent(base + h, kvd(h, r))
    sent(OZ, wo_buf.at[1, rows(piece, o_rows)])
    for i in range(7):
        sent(ONE + i, wo_at(1, 1, piece))
        sent(TWO + i, wo_at(2, 2, piece))
    for k in range(1, 4):
        sent(HOME + k, o_recv.at[k - 1])


def solution(mesh):
    def local_attn(x, w_query, w_key, w_value, w_out):
        d_model = x.shape[1]
        bf16, f32 = jnp.bfloat16, jnp.float32
        return pl.pallas_call(
            sublayer_kernel,
            out_shape=jax.ShapeDtypeStruct((HB, d_model), bf16),
            in_specs=[pl.BlockSpec(memory_space=pl.ANY)] * 5,
            out_specs=pl.BlockSpec(memory_space=pltpu.VMEM),
            scratch_shapes=[
                pltpu.VMEM((HB, d_model), f32),
                pltpu.VMEM((4, HB, d_model), bf16),
                pltpu.VMEM((d_model, 2 * HW), bf16),
                pltpu.VMEM((d_model, 2 * HW), bf16),
                pltpu.VMEM((4, HB, HW), bf16),
                pltpu.VMEM((16, HB, HW), bf16),
                pltpu.VMEM((3, 2, HB, HW), bf16),
                pltpu.VMEM((4, 2 * HB, 128), f32),
                pltpu.VMEM((4, 2 * HB, 128), f32),
                pltpu.VMEM((4, 2 * HB, HD), f32),
                pltpu.VMEM((4, HB, HW), bf16),
                pltpu.VMEM((3, HB, HW), bf16),
                pltpu.VMEM((4, HW, d_model), bf16),
                pltpu.SemaphoreType.DMA((N_TX,)),
                pltpu.SemaphoreType.DMA((N_TX,)),
                pltpu.SemaphoreType.DMA((5,)),
            ],
            compiler_params=pltpu.CompilerParams(collective_id=0, has_side_effects=True, vmem_limit_bytes=67043328),
            cost_estimate=pl.CostEstimate(flops=40_000_000_000, bytes_accessed=20_000_000, transcendentals=18_000_000),
            name="sublayer",
        )(x, w_key.reshape(d_model, HD), w_value.reshape(d_model, HD), w_query.reshape(d_model, HW), w_out.reshape(HW, d_model))

    return jax.shard_map(local_attn, mesh=mesh, in_specs=(P(("dp", "sp", "tp"), None), P(None, "tp", None), P(None, "tp", None), P(None, "tp", None), P("tp", None, None)), out_specs=P(("dp", "sp", "tp"), None), check_vma=False)
```

```python
import functools

import jax
import jax.numpy as jnp
from jax import lax
from jax.experimental import pallas as pl
from jax.experimental.pallas import tpu as pltpu
from jax.sharding import PartitionSpec as P

LOG2E = 1.4426950408889634
WINDOW = 4096
NEG_BIG = -1e30
MESH = pl.DeviceIdType.MESH

HB = 512
HD = 256
HW = 2 * HD
SUB = 256

_COUNT = (2, 1, 3, 1, 1, 1, 1, 4, 2, 2, 3, 3, 3, 3, 3, 3, 3, 3, 1, 7, 2, 2, 8, 4)
_START = [sum(_COUNT[:i]) for i in range(len(_COUNT))]
E1, C1, C2, WZ, WY, WX, WXY, WC, SHIP_KV, SHIP_Q, SHIPD_KV, SHIPD_Q, SP_Y, SP_OWN, SP_FAR, SPD_Y, SPD_OWN, SPD_FAR, OZ, ONE, OCROSS, OEDGE, TWO, HOME = _START
N_TX = sum(_COUNT)


def sublayer_kernel(x_ref, wk_ref, wv_ref, wq_ref, wo_ref, y_ref, y32, xbuf, wbuf, webuf, q_buf, kv_buf, made, m_ref, l_ref, acc_ref, o_buf, o_recv, wo_buf, send_sem, recv_sem, load_sem):
    z, r, dp = lax.axis_index("tp"), lax.axis_index("sp"), lax.axis_index("dp")
    z_by = (z, z + 1 - 2 * (z % 2), z + 2 - 4 * (z // 2), 3 - z)
    r1, r2 = r + 1 - 2 * (r % 2), r + 2 - 4 * (r // 2)
    inner = ((z + 1) // 2) % 2
    is_inner, is_edge = inner == 1, inner == 0
    d_model = xbuf.shape[2]
    w_rows, o_rows = d_model // 8, HW // 8

    t_c = inner * (3 - z) + (1 - inner) * z_by[2]
    t_d = inner * z_by[2] + (1 - inner) * (3 - z)
    t_of = (z, z_by[1], t_c, t_d)

    def half_id(t, rr):
        return t + 2 * rr + (t // 2) * (12 - 4 * rr)

    def to(**axes):
        return axes

    over_z = tuple(to(tp=z_by[k]) for k in range(4))
    over_core, over_y, over_x = to(sp=r1), to(sp=r2), to(dp=1 - dp)

    def tx(idx, src, dst, device):
        return pltpu.make_async_remote_copy(src_ref=src, dst_ref=dst, send_sem=send_sem.at[idx], recv_sem=recv_sem.at[idx], device_id=device, device_id_type=MESH)

    def send(idx, src, dst, device):
        tx(idx, src, dst, device).start()

    def arrived(idx, dst):
        tx(idx, dst, dst, over_core).wait_recv()

    def sent(idx, src):
        tx(idx, src, src, over_core).wait_send()

    def rows(n, size):
        return pl.ds(pl.multiple_of(n * size, size), size)

    x_half = [pl.ds(0, HB // 2), pl.ds(HB // 2, HB // 2)]
    x_part = [pl.ds(0, HB // 2), pl.ds(HB // 2, HB // 4), pl.ds(3 * HB // 4, HB // 4)]
    piece = dp * 4 + r
    p_y, p_x, p_xy = dp * 4 + r2, (1 - dp) * 4 + r, (1 - dp) * 4 + r2
    pieces_here = (piece, p_y, p_x, p_xy)
    pieces_mate = (dp * 4 + r1, dp * 4 + 3 - r, (1 - dp) * 4 + r1, (1 - dp) * 4 + 3 - r)

    def w_at(p):
        return webuf.at[rows(p, w_rows)]

    def wo_at(first, n, p):
        return wo_buf.at[pl.ds(first, n), rows(p, o_rows)]

    loads = [
        pltpu.make_async_copy(wk_ref, wbuf.at[:, 0:HD], load_sem.at[0]),
        pltpu.make_async_copy(wv_ref, wbuf.at[:, HD:HW], load_sem.at[1]),
        pltpu.make_async_copy(wq_ref, wbuf.at[:, HW:2 * HW], load_sem.at[2]),
        pltpu.make_async_copy(x_ref, xbuf.at[0], load_sem.at[3]),
        pltpu.make_async_copy(wo_ref, wo_buf.at[0], load_sem.at[4]),
    ]
    for c in loads:
        c.start()

    barrier = pltpu.get_barrier_semaphore()
    peers = over_z[1:] + (over_core, over_y, over_x)
    for peer in peers:
        pl.semaphore_signal(barrier, inc=1, device_id=peer, device_id_type=MESH)
    pl.semaphore_wait(barrier, len(peers))

    @pl.when(is_inner)
    def _():
        send(C1, x_ref, xbuf.at[2], over_z[3])

    for c in loads[:3]:
        c.wait()

    def out_edge():
        send(OZ, wo_ref.at[rows(piece, o_rows)], wo_buf.at[1, rows(piece, o_rows)], over_z[1])

    @pl.when(is_edge)
    def _():
        send(WZ, wbuf.at[rows(piece, w_rows)], w_at(piece), over_z[1])
        send(E1, x_ref.at[x_half[0]], xbuf.at[1, x_half[0]], over_z[1])
        out_edge()
        send(E1 + 1, x_ref.at[x_half[1]], xbuf.at[1, x_half[1]], over_z[1])

    @pl.when(is_inner)
    def _():
        out_edge()

    def project(slot, part, w, col0, dst):
        def step(n, carry):
            col = pl.multiple_of(n * HD, HD)
            res = jnp.dot(xbuf[slot, part, :], w[:, pl.ds(col0 + col, HD)], preferred_element_type=jnp.float32)
            dst[:, pl.ds(col, HD)] = res.astype(jnp.bfloat16)
            return carry

        lax.fori_loop(0, 2, step, 0)

    whole = pl.ds(0, HB)

    def kv_slot(j, rr):
        return kv_buf.at[half_id(t_of[j], rr)]

    def kvd(h, rr):
        return kv_buf.at[half_id(t_of[3], rr), x_part[h]]

    def spread(j):
        send(SP_Y + j, kv_slot(j, r), kv_slot(j, r), over_y)
        send(SP_OWN + j, kv_slot(j, r), kv_slot(j, r), over_core)

    def spread_on(j):
        arrived(SP_Y + j, kv_slot(j, r2))
        send(SP_FAR + j, kv_slot(j, r2), kv_slot(j, r2), over_core)

    def spread_wait(j):
        arrived(SP_OWN + j, kv_slot(j, r1))
        arrived(SP_FAR + j, kv_slot(j, 3 - r))

    def spread_last(h):
        send(SPD_Y + h, kvd(h, r), kvd(h, r), over_y)
        send(SPD_OWN + h, kvd(h, r), kvd(h, r), over_core)

    def spread_last_on(h):
        arrived(SPD_Y + h, kvd(h, r2))
        send(SPD_FAR + h, kvd(h, r2), kvd(h, r2), over_core)

    def spread_last_wait(h):
        arrived(SPD_OWN + h, kvd(h, r1))
        arrived(SPD_FAR + h, kvd(h, 3 - r))

    def own_heads(j):
        project(j, whole, wbuf, 0, kv_slot(j, r))
        project(j, whole, wbuf, HW, q_buf.at[t_of[j]])

    def edge_heads(i, j):
        t = t_of[j]
        project(j, whole, webuf, 0, made.at[i, 0])
        project(j, whole, webuf, HW, made.at[i, 1])
        send(SHIP_KV + i, made.at[i, 0], kv_buf.at[half_id(t, r)], over_z[1])
        send(SHIP_Q + i, made.at[i, 1], q_buf.at[t], over_z[1])

    def last_rows(h):
        part = x_part[h]
        arrived(C2 + h, xbuf.at[3, part])
        project(3, part, webuf, 0, made.at[2, 0, part])
        project(3, part, wbuf, 0, kvd(h, r))
        send(SHIPD_KV + h, made.at[2, 0, part], kvd(h, r), over_z[1])
        spread_last(h)
        project(3, part, webuf, HW, made.at[2, 1, part])
        project(3, part, wbuf, HW, q_buf.at[t_of[3], part])
        send(SHIPD_Q + h, made.at[2, 1, part], q_buf.at[t_of[3], part], over_z[1])

    def out_hop(base, first, n):
        send(base, wo_at(first, n, piece), wo_at(first, n, piece), over_x)
        send(base + 1, wo_at(first, n, piece), wo_at(first, n, piece), over_y)
        send(base + 3, wo_at(first, n, piece), wo_at(first, n, piece), over_core)

    def out_hop2(base, first, n):
        arrived(base + 1, wo_at(first, n, p_y))
        send(base + 2, wo_at(first, n, p_y), wo_at(first, n, p_y), over_x)
        send(base + 4, wo_at(first, n, p_y), wo_at(first, n, p_y), over_core)
        arrived(base, wo_at(first, n, p_x))
        send(base + 5, wo_at(first, n, p_x), wo_at(first, n, p_x), over_core)

    def out_hop3(base, first, n):
        arrived(base + 2, wo_at(first, n, p_xy))
        send(base + 6, wo_at(first, n, p_xy), wo_at(first, n, p_xy), over_core)

    def out_hop2_far():
        arrived(TWO + 1, wo_at(2, 2, p_y))
        send(TWO + 2, wo_at(2, 1, p_y), wo_at(2, 1, p_y), over_x)
        send(TWO + 4, wo_at(2, 2, p_y), wo_at(2, 2, p_y), over_core)
        arrived(TWO, wo_at(2, 2, p_x))
        send(TWO + 7, wo_at(3, 1, p_x), wo_at(3, 1, p_x), over_y)
        send(TWO + 5, wo_at(2, 2, p_x), wo_at(2, 2, p_x), over_core)

    def out_hop3_far():
        arrived(TWO + 2, wo_at(2, 1, p_xy))
        arrived(TWO + 7, wo_at(3, 1, p_xy))
        send(TWO + 6, wo_at(2, 2, p_xy), wo_at(2, 2, p_xy), over_core)

    def out_wait(base, first, n):
        for i in range(4):
            arrived(base + 3 + i, wo_at(first, n, pieces_mate[i]))

    loads[3].wait()
    own_heads(0)
    spread(0)
    m_ref[...] = jnp.full(m_ref.shape, NEG_BIG, jnp.float32)
    l_ref[...] = jnp.zeros(l_ref.shape, jnp.float32)
    acc_ref[...] = jnp.zeros(acc_ref.shape, jnp.float32)

    @pl.when(is_inner)
    def _():
        arrived(WZ, w_at(piece))
        send(WX, w_at(piece), w_at(piece), over_x)
        send(WY, w_at(piece), w_at(piece), over_y)
        send(WC, w_at(piece), w_at(piece), over_core)
        arrived(WY, w_at(p_y))
        send(WXY, w_at(p_y), w_at(p_y), over_x)
        send(WC + 1, w_at(p_y), w_at(p_y), over_core)
        arrived(WX, w_at(p_x))
        send(WC + 2, w_at(p_x), w_at(p_x), over_core)
        spread_on(0)
        arrived(E1, xbuf.at[1, x_half[0]])
        send(C2, xbuf.at[1, x_half[0]], xbuf.at[3, x_half[0]], over_z[3])
        arrived(WXY, w_at(p_xy))
        send(WC + 3, w_at(p_xy), w_at(p_xy), over_core)
        for i in range(4):
            arrived(WC + i, w_at(pieces_mate[i]))
        edge_heads(0, 0)
        arrived(OZ, wo_buf.at[1, rows(piece, o_rows)])
        out_hop(ONE, 1, 1)
        arrived(C1, xbuf.at[2])
        own_heads(2)
        spread(2)
        arrived(E1 + 1, xbuf.at[1, x_half[1]])
        for h in range(1, 3):
            send(C2 + h, xbuf.at[1, x_part[h]], xbuf.at[3, x_part[h]], over_z[3])
        send(OCROSS, wo_ref.at[rows(piece, o_rows)], wo_buf.at[3, rows(piece, o_rows)], over_z[3])
        send(OCROSS + 1, wo_buf.at[1, rows(piece, o_rows)], wo_buf.at[2, rows(piece, o_rows)], over_z[3])
        edge_heads(1, 2)
        own_heads(1)
        spread(1)
        spread_on(2)
        last_rows(0)
        spread_on(1)

    @pl.when(is_edge)
    def _():
        arrived(OZ, wo_buf.at[1, rows(piece, o_rows)])
        out_hop(ONE, 1, 1)
        spread_on(0)
        arrived(SHIP_KV, kv_slot(1, r))
        spread(1)
        arrived(SHIP_Q, q_buf.at[t_of[1]])
        spread_on(1)
        arrived(SHIP_KV + 1, kv_slot(2, r))
        spread(2)

    scale = LOG2E * HD ** -0.5

    def tile(t, g, gap, masked):
        k_blk = kv_buf[g, :, 0:HD]
        v_blk = kv_buf[g, :, HD:HW]
        n_sub = 2 * HB // SUB

        def scores(sub):
            head, off = divmod(sub * SUB, HB)
            q_sub = q_buf[t, pl.ds(off, SUB), head * HD:(head + 1) * HD]
            return lax.dot_general(q_sub, k_blk, (((1,), (1,)), ((), ())), preferred_element_type=jnp.float32)

        ahead = scores(0)
        for sub in range(n_sub):
            off = sub * SUB % HB
            rs = pl.ds(sub * SUB, SUB)
            s = ahead
            if sub + 1 < n_sub:
                ahead = scores(sub + 1)
            if masked:
                dist = gap * HB + off + lax.broadcasted_iota(jnp.int32, (SUB, HB), 0) - lax.broadcasted_iota(jnp.int32, (SUB, HB), 1)
                s = jnp.where((dist >= 0) & (dist < WINDOW), s, -jnp.inf)
            m_old = m_ref[t, rs, :]
            m_new = jnp.maximum(m_old, jnp.max(s, axis=1, keepdims=True))
            alpha = jnp.exp2((m_old - m_new) * scale)
            p = jnp.exp2((s - jnp.concatenate([m_new] * 4, axis=1)) * scale)
            l_new = p[:, 0:128] + p[:, 128:256] + p[:, 256:384] + p[:, 384:512]
            pv = jnp.dot(p.astype(jnp.bfloat16), v_blk, preferred_element_type=jnp.float32)
            m_ref[t, rs, :] = m_new
            l_ref[t, rs, :] = l_ref[t, rs, :] * alpha + l_new
            acc_ref[t, rs, :] = acc_ref[t, rs, :] * jnp.concatenate([alpha, alpha], axis=1) + pv

    def pick(j):
        return (j == 0) * t_of[0] + (j == 1) * t_of[1] + (j == 2) * t_of[2] + (j == 3) * t_of[3]

    def attend(n, combo):
        def step(i, carry):
            jq, jk = combo(i // 4)
            t = pick(jq)
            g = half_id(pick(jk), i % 4)
            gap = half_id(t, r) - g

            @pl.when((gap > 0) & (gap < 8))
            def _():
                tile(t, g, gap, False)

            @pl.when((gap == 0) | (gap == 8))
            def _():
                tile(t, g, gap, True)

            return carry

        lax.fori_loop(0, 4 * n, step, 0)

    def finish(t):
        for sub in range(2 * HB // SUB):
            head, off = divmod(sub * SUB, HB)
            rs = pl.ds(sub * SUB, SUB)
            total = jnp.sum(l_ref[t, rs, :], axis=1, keepdims=True)
            o_buf[t, pl.ds(off, SUB), head * HD:(head + 1) * HD] = (acc_ref[t, rs, :] / total).astype(jnp.bfloat16)

    spread_wait(0)
    spread_wait(1)
    attend(4 * (1 - inner), lambda i: (i % 2, i // 2))

    @pl.when(is_edge)
    def _():
        arrived(SHIPD_KV, kvd(0, r))
        spread_last(0)
        spread_on(2)
        arrived(SHIP_Q + 1, q_buf.at[t_of[2]])

    out_hop2(ONE, 1, 1)
    spread_wait(2)
    attend(3, lambda i: (2, i))
    spread_last_on(0)

    @pl.when(is_inner)
    def _():
        last_rows(1)
        last_rows(2)

    @pl.when(is_edge)
    def _():
        for h in range(1, 3):
            arrived(SHIPD_KV + h, kvd(h, r))
            spread_last(h)

    out_hop3(ONE, 1, 1)
    spread_last_on(1)
    attend(3 * inner, lambda i: (3, i))
    spread_last_on(2)
    for h in range(3):
        spread_last_wait(h)
    attend(1, lambda i: (2, 3))
    finish(t_c)

    def home(t, by_inner, by_edge):
        @pl.when(is_inner)
        def _():
            send(HOME + by_inner, o_buf.at[t], o_recv.at[by_inner - 1], over_z[by_inner])

        @pl.when(is_edge)
        def _():
            send(HOME + by_edge, o_buf.at[t], o_recv.at[by_edge - 1], over_z[by_edge])

    home(t_c, 3, 2)

    @pl.when(is_inner)
    def _():
        for i in range(2):
            arrived(OCROSS + i, wo_buf.at[3 - i, rows(piece, o_rows)])
            send(OEDGE + i, wo_buf.at[3 - i, rows(piece, o_rows)], wo_buf.at[2 + i, rows(piece, o_rows)], over_z[1])

    @pl.when(is_edge)
    def _():
        for h in range(3):
            arrived(SHIPD_Q + h, q_buf.at[t_of[3], x_part[h]])

    attend(4 - 3 * inner, lambda i: (3, (i + 3) % 4))
    finish(t_d)
    home(t_d, 2, 3)

    @pl.when(is_edge)
    def _():
        for i in range(2):
            arrived(OEDGE + i, wo_buf.at[2 + i, rows(piece, o_rows)])

    out_hop(TWO, 2, 2)
    attend(4 + 4 * inner, lambda i: (i % 2, (i // 2 + 2) % 4))
    finish(z_by[1])
    finish(z)
    send(HOME + 1, o_buf.at[z_by[1]], o_recv.at[0], over_z[1])
    out_hop2_far()
    loads[4].wait()

    def out_own(n, carry):
        cols = rows(n, HD)
        y32[:, cols] = jnp.dot(o_buf[z], wo_buf[0, :, cols], preferred_element_type=jnp.float32)
        return carry

    lax.fori_loop(0, d_model // HD, out_own, 0)
    out_hop3_far()
    out_wait(ONE, 1, 1)
    arrived(HOME + 1, o_recv.at[0])

    def out_near(n, carry):
        cols = rows(n, HD)
        y32[:, cols] = y32[:, cols] + jnp.dot(o_recv[0], wo_buf[1, :, cols], preferred_element_type=jnp.float32)
        return carry

    lax.fori_loop(0, d_model // HD, out_near, 0)
    out_wait(TWO, 2, 2)
    for k in range(2, 4):
        arrived(HOME + k, o_recv.at[k - 1])

    def out_far(n, carry):
        cols = rows(n, HD)
        far = jnp.dot(o_recv[1], wo_buf[2, :, cols], preferred_element_type=jnp.float32)
        far = far + jnp.dot(o_recv[2], wo_buf[3, :, cols], preferred_element_type=jnp.float32)
        y_ref[:, cols] = (y32[:, cols] + far).astype(jnp.bfloat16)
        return carry

    lax.fori_loop(0, d_model // HD, out_far, 0)

    @pl.when(is_edge)
    def _():
        sent(WZ, w_at(piece))
        for h in range(2):
            sent(E1 + h, xbuf.at[1, x_half[h]])

    @pl.when(is_inner)
    def _():
        sent(C1, xbuf.at[2])
        for h in range(3):
            sent(C2 + h, xbuf.at[3, x_part[h]])
            sent(SHIPD_KV + h, made.at[2, 0, x_part[h]])
            sent(SHIPD_Q + h, made.at[2, 1, x_part[h]])
        for h in range(2):
            sent(SHIP_KV + h, made.at[h, 0])
            sent(SHIP_Q + h, made.at[h, 1])
            sent(OCROSS + h, wo_buf.at[2 + h, rows(piece, o_rows)])
            sent(OEDGE + h, wo_buf.at[2 + h, rows(piece, o_rows)])
        for idx in (WY, WX, WXY, WC, WC + 1, WC + 2, WC + 3):
            sent(idx, w_at(piece))

    for j in range(3):
        for base in (SP_Y, SP_OWN, SP_FAR):
            sent(base + j, kv_slot(j, r))
    for h in range(3):
        for base in (SPD_Y, SPD_OWN, SPD_FAR):
            sent(base + h, kvd(h, r))
    sent(OZ, wo_buf.at[1, rows(piece, o_rows)])
    for i in range(7):
        sent(ONE + i, wo_at(1, 1, piece))
    for i in range(8):
        sent(TWO + i, wo_at(2, 1 if i in (2, 7) else 2, piece))
    for k in range(1, 4):
        sent(HOME + k, o_recv.at[k - 1])


def solution(mesh):
    def local_attn(x, w_query, w_key, w_value, w_out):
        d_model = x.shape[1]
        bf16, f32 = jnp.bfloat16, jnp.float32
        return pl.pallas_call(
            sublayer_kernel,
            out_shape=jax.ShapeDtypeStruct((HB, d_model), bf16),
            in_specs=[pl.BlockSpec(memory_space=pl.ANY)] * 5,
            out_specs=pl.BlockSpec(memory_space=pltpu.VMEM),
            scratch_shapes=[
                pltpu.VMEM((HB, d_model), f32),
                pltpu.VMEM((4, HB, d_model), bf16),
                pltpu.VMEM((d_model, 2 * HW), bf16),
                pltpu.VMEM((d_model, 2 * HW), bf16),
                pltpu.VMEM((4, HB, HW), bf16),
                pltpu.VMEM((16, HB, HW), bf16),
                pltpu.VMEM((3, 2, HB, HW), bf16),
                pltpu.VMEM((4, 2 * HB, 128), f32),
                pltpu.VMEM((4, 2 * HB, 128), f32),
                pltpu.VMEM((4, 2 * HB, HD), f32),
                pltpu.VMEM((4, HB, HW), bf16),
                pltpu.VMEM((3, HB, HW), bf16),
                pltpu.VMEM((4, HW, d_model), bf16),
                pltpu.SemaphoreType.DMA((N_TX,)),
                pltpu.SemaphoreType.DMA((N_TX,)),
                pltpu.SemaphoreType.DMA((5,)),
            ],
            compiler_params=pltpu.CompilerParams(collective_id=0, has_side_effects=True, vmem_limit_bytes=67043328),
            cost_estimate=pl.CostEstimate(flops=40_000_000_000, bytes_accessed=20_000_000, transcendentals=18_000_000),
            name="sublayer",
        )(x, w_key.reshape(d_model, HD), w_value.reshape(d_model, HD), w_query.reshape(d_model, HW), w_out.reshape(HW, d_model))

    return jax.shard_map(local_attn, mesh=mesh, in_specs=(P(("dp", "sp", "tp"), None), P(None, "tp", None), P(None, "tp", None), P(None, "tp", None), P("tp", None, None)), out_specs=P(("dp", "sp", "tp"), None), check_vma=False)
```

```python
import functools

import jax
import jax.numpy as jnp
from jax import lax
from jax.experimental import pallas as pl
from jax.experimental.pallas import tpu as pltpu
from jax.sharding import PartitionSpec as P

LOG2E = 1.4426950408889634
WINDOW = 4096
NEG_BIG = -1e30
MESH = pl.DeviceIdType.MESH

HB = 512
HD = 256
HW = 2 * HD
SUB = 256

_COUNT = (2, 1, 3, 1, 1, 1, 1, 4, 2, 2, 3, 3, 3, 3, 3, 3, 3, 3, 1, 7, 2, 2, 8, 4)
_START = [sum(_COUNT[:i]) for i in range(len(_COUNT))]
E1, C1, C2, WZ, WY, WX, WXY, WC, SHIP_KV, SHIP_Q, SHIPD_KV, SHIPD_Q, SP_Y, SP_OWN, SP_FAR, SPD_Y, SPD_OWN, SPD_FAR, OZ, ONE, OCROSS, OEDGE, TWO, HOME = _START
N_TX = sum(_COUNT)


def sublayer_kernel(x_ref, wk_ref, wv_ref, wq_ref, wo_ref, y_ref, y32, xbuf, wbuf, webuf, q_buf, kv_buf, made, m_ref, l_ref, acc_ref, o_buf, o_recv, wo_buf, send_sem, recv_sem, load_sem):
    z, r, dp = lax.axis_index("tp"), lax.axis_index("sp"), lax.axis_index("dp")
    z_by = (z, z + 1 - 2 * (z % 2), z + 2 - 4 * (z // 2), 3 - z)
    r1, r2 = r + 1 - 2 * (r % 2), r + 2 - 4 * (r // 2)
    inner = ((z + 1) // 2) % 2
    is_inner, is_edge = inner == 1, inner == 0
    d_model = xbuf.shape[2]
    w_rows, o_rows = d_model // 8, HW // 8

    t_c = inner * (3 - z) + (1 - inner) * z_by[2]
    t_d = inner * z_by[2] + (1 - inner) * (3 - z)
    t_of = (z, z_by[1], t_c, t_d)

    def half_id(t, rr):
        return t + 2 * rr + (t // 2) * (12 - 4 * rr)

    def to(**axes):
        return axes

    over_z = tuple(to(tp=z_by[k]) for k in range(4))
    over_core, over_y, over_x = to(sp=r1), to(sp=r2), to(dp=1 - dp)

    def tx(idx, src, dst, device):
        return pltpu.make_async_remote_copy(src_ref=src, dst_ref=dst, send_sem=send_sem.at[idx], recv_sem=recv_sem.at[idx], device_id=device, device_id_type=MESH)

    def send(idx, src, dst, device):
        tx(idx, src, dst, device).start()

    def arrived(idx, dst):
        tx(idx, dst, dst, over_core).wait_recv()

    def sent(idx, src):
        tx(idx, src, src, over_core).wait_send()

    def rows(n, size):
        return pl.ds(pl.multiple_of(n * size, size), size)

    x_half = [pl.ds(0, HB // 2), pl.ds(HB // 2, HB // 2)]
    x_part = [pl.ds(0, HB // 2), pl.ds(HB // 2, HB // 4), pl.ds(3 * HB // 4, HB // 4)]
    piece = dp * 4 + r
    p_y, p_x, p_xy = dp * 4 + r2, (1 - dp) * 4 + r, (1 - dp) * 4 + r2
    pieces_here = (piece, p_y, p_x, p_xy)
    pieces_mate = (dp * 4 + r1, dp * 4 + 3 - r, (1 - dp) * 4 + r1, (1 - dp) * 4 + 3 - r)

    def w_at(p):
        return webuf.at[rows(p, w_rows)]

    def wo_at(first, n, p):
        return wo_buf.at[pl.ds(first, n), rows(p, o_rows)]

    loads = [
        pltpu.make_async_copy(wk_ref, wbuf.at[:, 0:HD], load_sem.at[0]),
        pltpu.make_async_copy(wv_ref, wbuf.at[:, HD:HW], load_sem.at[1]),
        pltpu.make_async_copy(wq_ref, wbuf.at[:, HW:2 * HW], load_sem.at[2]),
        pltpu.make_async_copy(x_ref, xbuf.at[0], load_sem.at[3]),
        pltpu.make_async_copy(wo_ref, wo_buf.at[0], load_sem.at[4]),
    ]
    for c in loads:
        c.start()

    barrier = pltpu.get_barrier_semaphore()
    peers = over_z[1:] + (over_core, over_y, over_x)
    for peer in peers:
        pl.semaphore_signal(barrier, inc=1, device_id=peer, device_id_type=MESH)
    pl.semaphore_wait(barrier, len(peers))

    @pl.when(is_inner)
    def _():
        send(C1, x_ref, xbuf.at[2], over_z[3])

    for c in loads[:3]:
        c.wait()

    def out_edge():
        send(OZ, wo_ref.at[rows(piece, o_rows)], wo_buf.at[1, rows(piece, o_rows)], over_z[1])

    @pl.when(is_edge)
    def _():
        send(WZ, wbuf.at[rows(piece, w_rows)], w_at(piece), over_z[1])
        send(E1, x_ref.at[x_half[0]], xbuf.at[1, x_half[0]], over_z[1])
        out_edge()
        send(E1 + 1, x_ref.at[x_half[1]], xbuf.at[1, x_half[1]], over_z[1])

    @pl.when(is_inner)
    def _():
        out_edge()

    def project(slot, part, w, col0, dst):
        def step(n, carry):
            col = pl.multiple_of(n * HD, HD)
            res = jnp.dot(xbuf[slot, part, :], w[:, pl.ds(col0 + col, HD)], preferred_element_type=jnp.float32)
            dst[:, pl.ds(col, HD)] = res.astype(jnp.bfloat16)
            return carry

        lax.fori_loop(0, 2, step, 0)

    whole = pl.ds(0, HB)

    def kv_slot(j, rr):
        return kv_buf.at[half_id(t_of[j], rr)]

    def kvd(h, rr):
        return kv_buf.at[half_id(t_of[3], rr), x_part[h]]

    def spread(j):
        send(SP_Y + j, kv_slot(j, r), kv_slot(j, r), over_y)
        send(SP_OWN + j, kv_slot(j, r), kv_slot(j, r), over_core)

    def spread_on(j):
        arrived(SP_Y + j, kv_slot(j, r2))
        send(SP_FAR + j, kv_slot(j, r2), kv_slot(j, r2), over_core)

    def spread_wait(j):
        arrived(SP_OWN + j, kv_slot(j, r1))
        arrived(SP_FAR + j, kv_slot(j, 3 - r))

    def spread_last(h):
        send(SPD_Y + h, kvd(h, r), kvd(h, r), over_y)
        send(SPD_OWN + h, kvd(h, r), kvd(h, r), over_core)

    def spread_last_on(h):
        arrived(SPD_Y + h, kvd(h, r2))
        send(SPD_FAR + h, kvd(h, r2), kvd(h, r2), over_core)

    def spread_last_wait(h):
        arrived(SPD_OWN + h, kvd(h, r1))
        arrived(SPD_FAR + h, kvd(h, 3 - r))

    def own_heads(j):
        project(j, whole, wbuf, 0, kv_slot(j, r))
        project(j, whole, wbuf, HW, q_buf.at[t_of[j]])

    def edge_heads(i, j):
        t = t_of[j]
        project(j, whole, webuf, 0, made.at[i, 0])
        project(j, whole, webuf, HW, made.at[i, 1])
        send(SHIP_KV + i, made.at[i, 0], kv_buf.at[half_id(t, r)], over_z[1])
        send(SHIP_Q + i, made.at[i, 1], q_buf.at[t], over_z[1])

    def last_rows(h):
        part = x_part[h]
        arrived(C2 + h, xbuf.at[3, part])
        project(3, part, webuf, 0, made.at[2, 0, part])
        project(3, part, wbuf, 0, kvd(h, r))
        send(SHIPD_KV + h, made.at[2, 0, part], kvd(h, r), over_z[1])
        spread_last(h)
        project(3, part, webuf, HW, made.at[2, 1, part])
        project(3, part, wbuf, HW, q_buf.at[t_of[3], part])
        send(SHIPD_Q + h, made.at[2, 1, part], q_buf.at[t_of[3], part], over_z[1])

    def out_hop(base, first, n):
        send(base, wo_at(first, n, piece), wo_at(first, n, piece), over_x)
        send(base + 1, wo_at(first, n, piece), wo_at(first, n, piece), over_y)
        send(base + 3, wo_at(first, n, piece), wo_at(first, n, piece), over_core)

    def out_hop2(base, first, n):
        arrived(base + 1, wo_at(first, n, p_y))
        send(base + 2, wo_at(first, n, p_y), wo_at(first, n, p_y), over_x)
        send(base + 4, wo_at(first, n, p_y), wo_at(first, n, p_y), over_core)
        arrived(base, wo_at(first, n, p_x))
        send(base + 5, wo_at(first, n, p_x), wo_at(first, n, p_x), over_core)

    def out_hop3(base, first, n):
        arrived(base + 2, wo_at(first, n, p_xy))
        send(base + 6, wo_at(first, n, p_xy), wo_at(first, n, p_xy), over_core)

    def out_hop2_far():
        arrived(TWO + 1, wo_at(2, 2, p_y))
        send(TWO + 2, wo_at(2, 1, p_y), wo_at(2, 1, p_y), over_x)
        send(TWO + 4, wo_at(2, 2, p_y), wo_at(2, 2, p_y), over_core)
        arrived(TWO, wo_at(2, 2, p_x))
        send(TWO + 7, wo_at(3, 1, p_x), wo_at(3, 1, p_x), over_y)
        send(TWO + 5, wo_at(2, 2, p_x), wo_at(2, 2, p_x), over_core)

    def out_hop3_far():
        arrived(TWO + 2, wo_at(2, 1, p_xy))
        arrived(TWO + 7, wo_at(3, 1, p_xy))
        send(TWO + 6, wo_at(2, 2, p_xy), wo_at(2, 2, p_xy), over_core)

    def out_wait(base, first, n):
        for i in range(4):
            arrived(base + 3 + i, wo_at(first, n, pieces_mate[i]))

    loads[3].wait()
    own_heads(0)
    spread(0)
    m_ref[...] = jnp.full(m_ref.shape, NEG_BIG, jnp.float32)
    l_ref[...] = jnp.zeros(l_ref.shape, jnp.float32)
    acc_ref[...] = jnp.zeros(acc_ref.shape, jnp.float32)

    @pl.when(is_inner)
    def _():
        arrived(WZ, w_at(piece))
        send(WX, w_at(piece), w_at(piece), over_x)
        send(WY, w_at(piece), w_at(piece), over_y)
        send(WC, w_at(piece), w_at(piece), over_core)
        arrived(WY, w_at(p_y))
        send(WXY, w_at(p_y), w_at(p_y), over_x)
        send(WC + 1, w_at(p_y), w_at(p_y), over_core)
        arrived(WX, w_at(p_x))
        send(WC + 2, w_at(p_x), w_at(p_x), over_core)
        spread_on(0)
        arrived(E1, xbuf.at[1, x_half[0]])
        send(C2, xbuf.at[1, x_half[0]], xbuf.at[3, x_half[0]], over_z[3])
        arrived(WXY, w_at(p_xy))
        send(WC + 3, w_at(p_xy), w_at(p_xy), over_core)
        for i in range(4):
            arrived(WC + i, w_at(pieces_mate[i]))
        edge_heads(0, 0)
        arrived(OZ, wo_buf.at[1, rows(piece, o_rows)])
        out_hop(ONE, 1, 1)
        arrived(C1, xbuf.at[2])
        own_heads(2)
        spread(2)
        arrived(E1 + 1, xbuf.at[1, x_half[1]])
        for h in range(1, 3):
            send(C2 + h, xbuf.at[1, x_part[h]], xbuf.at[3, x_part[h]], over_z[3])
        send(OCROSS, wo_ref.at[rows(piece, o_rows)], wo_buf.at[3, rows(piece, o_rows)], over_z[3])
        send(OCROSS + 1, wo_buf.at[1, rows(piece, o_rows)], wo_buf.at[2, rows(piece, o_rows)], over_z[3])
        edge_heads(1, 2)
        own_heads(1)
        spread(1)
        spread_on(2)
        last_rows(0)
        spread_on(1)

    @pl.when(is_edge)
    def _():
        arrived(OZ, wo_buf.at[1, rows(piece, o_rows)])
        out_hop(ONE, 1, 1)
        spread_on(0)
        arrived(SHIP_KV, kv_slot(1, r))
        spread(1)
        arrived(SHIP_Q, q_buf.at[t_of[1]])
        spread_on(1)
        arrived(SHIP_KV + 1, kv_slot(2, r))
        spread(2)

    scale = LOG2E * HD ** -0.5

    def tile(t, g, gap, masked):
        k_blk = kv_buf[g, :, 0:HD]
        v_blk = kv_buf[g, :, HD:HW]
        n_sub = 2 * HB // SUB

        def scores(sub):
            head, off = divmod(sub * SUB, HB)
            q_sub = q_buf[t, pl.ds(off, SUB), head * HD:(head + 1) * HD]
            return lax.dot_general(q_sub, k_blk, (((1,), (1,)), ((), ())), preferred_element_type=jnp.float32)

        ahead = scores(0)
        for sub in range(n_sub):
            off = sub * SUB % HB
            rs = pl.ds(sub * SUB, SUB)
            s = ahead
            if sub + 1 < n_sub:
                ahead = scores(sub + 1)
            if masked:
                dist = gap * HB + off + lax.broadcasted_iota(jnp.int32, (SUB, HB), 0) - lax.broadcasted_iota(jnp.int32, (SUB, HB), 1)
                s = jnp.where((dist >= 0) & (dist < WINDOW), s, -jnp.inf)
            m_old = m_ref[t, rs, :]
            m_new = jnp.maximum(m_old, jnp.max(s, axis=1, keepdims=True))
            alpha = jnp.exp2((m_old - m_new) * scale)
            p = jnp.exp2((s - jnp.concatenate([m_new] * 4, axis=1)) * scale)
            l_new = p[:, 0:128] + p[:, 128:256] + p[:, 256:384] + p[:, 384:512]
            pv = jnp.dot(p.astype(jnp.bfloat16), v_blk, preferred_element_type=jnp.float32)
            m_ref[t, rs, :] = m_new
            l_ref[t, rs, :] = l_ref[t, rs, :] * alpha + l_new
            acc_ref[t, rs, :] = acc_ref[t, rs, :] * jnp.concatenate([alpha, alpha], axis=1) + pv

    def pick(j):
        return (j == 0) * t_of[0] + (j == 1) * t_of[1] + (j == 2) * t_of[2] + (j == 3) * t_of[3]

    def attend(n, combo):
        def step(i, carry):
            jq, jk = combo(i // 4)
            t = pick(jq)
            g = half_id(pick(jk), i % 4)
            gap = half_id(t, r) - g

            @pl.when((gap > 0) & (gap < 8))
            def _():
                tile(t, g, gap, False)

            @pl.when((gap == 0) | (gap == 8))
            def _():
                tile(t, g, gap, True)

            return carry

        lax.fori_loop(0, 4 * n, step, 0)

    def finish(t):
        for sub in range(2 * HB // SUB):
            head, off = divmod(sub * SUB, HB)
            rs = pl.ds(sub * SUB, SUB)
            total = jnp.sum(l_ref[t, rs, :], axis=1, keepdims=True)
            o_buf[t, pl.ds(off, SUB), head * HD:(head + 1) * HD] = (acc_ref[t, rs, :] / total).astype(jnp.bfloat16)

    spread_wait(0)
    spread_wait(1)
    attend(4 * (1 - inner), lambda i: (i % 2, i // 2))

    @pl.when(is_edge)
    def _():
        arrived(SHIPD_KV, kvd(0, r))
        spread_last(0)
        spread_on(2)
        arrived(SHIP_Q + 1, q_buf.at[t_of[2]])

    out_hop2(ONE, 1, 1)
    spread_wait(2)
    attend(3, lambda i: (2, i))
    spread_last_on(0)

    @pl.when(is_inner)
    def _():
        last_rows(1)
        last_rows(2)

    @pl.when(is_edge)
    def _():
        for h in range(1, 3):
            arrived(SHIPD_KV + h, kvd(h, r))
            spread_last(h)

    out_hop3(ONE, 1, 1)
    spread_last_on(1)
    attend(3 * inner, lambda i: (3, i))
    spread_last_on(2)
    for h in range(3):
        spread_last_wait(h)
    attend(1, lambda i: (2, 3))
    finish(t_c)

    def home(t, by_inner, by_edge):
        @pl.when(is_inner)
        def _():
            send(HOME + by_inner, o_buf.at[t], o_recv.at[by_inner - 1], over_z[by_inner])

        @pl.when(is_edge)
        def _():
            send(HOME + by_edge, o_buf.at[t], o_recv.at[by_edge - 1], over_z[by_edge])

    home(t_c, 3, 2)

    @pl.when(is_inner)
    def _():
        for i in range(2):
            arrived(OCROSS + i, wo_buf.at[3 - i, rows(piece, o_rows)])
            send(OEDGE + i, wo_buf.at[3 - i, rows(piece, o_rows)], wo_buf.at[2 + i, rows(piece, o_rows)], over_z[1])

    @pl.when(is_edge)
    def _():
        for h in range(3):
            arrived(SHIPD_Q + h, q_buf.at[t_of[3], x_part[h]])

    attend(4 - 3 * inner, lambda i: (3, (i + 3) % 4))
    finish(t_d)
    home(t_d, 2, 3)

    @pl.when(is_edge)
    def _():
        for i in range(2):
            arrived(OEDGE + i, wo_buf.at[2 + i, rows(piece, o_rows)])

    out_hop(TWO, 2, 2)
    attend(4 + 4 * inner, lambda i: (i % 2, (i // 2 + 2) % 4))
    finish(z_by[1])
    finish(z)
    send(HOME + 1, o_buf.at[z_by[1]], o_recv.at[0], over_z[1])
    out_hop2_far()
    loads[4].wait()

    wide = 3 * HD

    def out_add(o_ref, k, first):
        def step(n, carry):
            cols = rows(n, wide)
            part = jnp.dot(o_ref[...], wo_buf[k, :, cols], preferred_element_type=jnp.float32)
            y32[:, cols] = part if first else y32[:, cols] + part
            return carry

        lax.fori_loop(0, d_model // wide, step, 0)

    out_add(o_buf.at[z], 0, True)
    out_hop3_far()
    out_wait(ONE, 1, 1)
    arrived(HOME + 1, o_recv.at[0])
    out_add(o_recv.at[0], 1, False)
    out_wait(TWO, 2, 2)

    @pl.when(is_inner)
    def _():
        arrived(HOME + 3, o_recv.at[2])

    @pl.when(is_edge)
    def _():
        arrived(HOME + 2, o_recv.at[1])

    out_add(o_recv.at[1 + inner], 2 + inner, False)

    @pl.when(is_inner)
    def _():
        arrived(HOME + 2, o_recv.at[1])

    @pl.when(is_edge)
    def _():
        arrived(HOME + 3, o_recv.at[2])

    def out_last(n, carry):
        cols = rows(n, wide)
        part = jnp.dot(o_recv[2 - inner], wo_buf[3 - inner, :, cols], preferred_element_type=jnp.float32)
        y_ref[:, cols] = (y32[:, cols] + part).astype(jnp.bfloat16)
        return carry

    lax.fori_loop(0, d_model // wide, out_last, 0)

    @pl.when(is_edge)
    def _():
        sent(WZ, w_at(piece))
        for h in range(2):
            sent(E1 + h, xbuf.at[1, x_half[h]])

    @pl.when(is_inner)
    def _():
        sent(C1, xbuf.at[2])
        for h in range(3):
            sent(C2 + h, xbuf.at[3, x_part[h]])
            sent(SHIPD_KV + h, made.at[2, 0, x_part[h]])
            sent(SHIPD_Q + h, made.at[2, 1, x_part[h]])
        for h in range(2):
            sent(SHIP_KV + h, made.at[h, 0])
            sent(SHIP_Q + h, made.at[h, 1])
            sent(OCROSS + h, wo_buf.at[2 + h, rows(piece, o_rows)])
            sent(OEDGE + h, wo_buf.at[2 + h, rows(piece, o_rows)])
        for idx in (WY, WX, WXY, WC, WC + 1, WC + 2, WC + 3):
            sent(idx, w_at(piece))

    for j in range(3):
        for base in (SP_Y, SP_OWN, SP_FAR):
            sent(base + j, kv_slot(j, r))
    for h in range(3):
        for base in (SPD_Y, SPD_OWN, SPD_FAR):
            sent(base + h, kvd(h, r))
    sent(OZ, wo_buf.at[1, rows(piece, o_rows)])
    for i in range(7):
        sent(ONE + i, wo_at(1, 1, piece))
    for i in range(8):
        sent(TWO + i, wo_at(2, 1 if i in (2, 7) else 2, piece))
    for k in range(1, 4):
        sent(HOME + k, o_recv.at[k - 1])


def solution(mesh):
    def local_attn(x, w_query, w_key, w_value, w_out):
        d_model = x.shape[1]
        bf16, f32 = jnp.bfloat16, jnp.float32
        return pl.pallas_call(
            sublayer_kernel,
            out_shape=jax.ShapeDtypeStruct((HB, d_model), bf16),
            in_specs=[pl.BlockSpec(memory_space=pl.ANY)] * 5,
            out_specs=pl.BlockSpec(memory_space=pltpu.VMEM),
            scratch_shapes=[
                pltpu.VMEM((HB, d_model), f32),
                pltpu.VMEM((4, HB, d_model), bf16),
                pltpu.VMEM((d_model, 2 * HW), bf16),
                pltpu.VMEM((d_model, 2 * HW), bf16),
                pltpu.VMEM((4, HB, HW), bf16),
                pltpu.VMEM((16, HB, HW), bf16),
                pltpu.VMEM((3, 2, HB, HW), bf16),
                pltpu.VMEM((4, 2 * HB, 128), f32),
                pltpu.VMEM((4, 2 * HB, 128), f32),
                pltpu.VMEM((4, 2 * HB, HD), f32),
                pltpu.VMEM((4, HB, HW), bf16),
                pltpu.VMEM((3, HB, HW), bf16),
                pltpu.VMEM((4, HW, d_model), bf16),
                pltpu.SemaphoreType.DMA((N_TX,)),
                pltpu.SemaphoreType.DMA((N_TX,)),
                pltpu.SemaphoreType.DMA((5,)),
            ],
            compiler_params=pltpu.CompilerParams(collective_id=0, has_side_effects=True, vmem_limit_bytes=67043328),
            cost_estimate=pl.CostEstimate(flops=40_000_000_000, bytes_accessed=20_000_000, transcendentals=18_000_000),
            name="sublayer",
        )(x, w_key.reshape(d_model, HD), w_value.reshape(d_model, HD), w_query.reshape(d_model, HW), w_out.reshape(HW, d_model))

    return jax.shard_map(local_attn, mesh=mesh, in_specs=(P(("dp", "sp", "tp"), None), P(None, "tp", None), P(None, "tp", None), P(None, "tp", None), P("tp", None, None)), out_specs=P(("dp", "sp", "tp"), None), check_vma=False)
```
